256 devices in a mesh: member: 4 (over x, y), region: 64 (over z, core).
Axes of the slice: x: 2, y: 2, z: 32, core: 2. Of those that a mesh axis runs over, the one named last changes fastest.
The devices are a block of a 4x8x32 slice.
Arguments:
- mesh_nodes: bfloat16 [131072, 512], P(('member', 'region')), parts along dimension 0, may hold values from -6 to 6
- mesh_edges: bfloat16 [131072, 512], P('region'), may hold values from -6 to 6
- grid_nodes: bfloat16 [98304, 512], P(('member', 'region')), parts along dimension 0, may hold values from -6 to 6
- grid_edges: bfloat16 [73728, 512], P('region'), may hold values from -6 to 6
- boundary: int32 [64, 32], P('region'), may hold values from 0 to 511
- mesh_need: int32 [64, 64, 8], P('region'), may hold values from 0 to 31
- mesh_sender: int32 [64, 2048], P('region'), may hold values from 0 to 1023, as said below
- mesh_receiver: int32 [64, 2048], P('region'), may hold values from 0 to 511
- mesh_live: int32 [64], P('region'), may hold values from 512 to 2048, as said below
- grid_need: int32 [64, 4, 8], P('region'), may hold values from 0 to 31
- grid_sender: int32 [64, 1152], P('region'), may hold values from 0 to 543, as said below
- grid_receiver: int32 [64, 1152], P('region'), may hold values from 0 to 383
- process_edge_in: bfloat16 [1536, 512], replicated, may hold values from -0.15625 to 0.15625
- process_edge_bias: float32 [512], replicated, may hold values from -3 to 3
- process_edge_out: bfloat16 [512, 512], replicated, may hold values from -0.25 to 0.25
- process_edge_gain: float32 [512], replicated, may hold values from 0.5 to 1.5
- process_node_in: bfloat16 [1024, 512], replicated, may hold values from -0.1875 to 0.1875
- process_node_bias: float32 [512], replicated, may hold values from -3 to 3
- process_node_out: bfloat16 [512, 512], replicated, may hold values from -0.25 to 0.25
- process_node_gain: float32 [512], replicated, may hold values from 0.5 to 1.5
- decode_edge_in: bfloat16 [1536, 512], replicated, may hold values from -0.15625 to 0.15625
- decode_edge_bias: float32 [512], replicated, may hold values from -3 to 3
- decode_edge_out: bfloat16 [512, 512], replicated, may hold values from -0.25 to 0.25
- decode_edge_gain: float32 [512], replicated, may hold values from 0.5 to 1.5
- decode_node_in: bfloat16 [1024, 512], replicated, may hold values from -0.1875 to 0.1875
- decode_node_bias: float32 [512], replicated, may hold values from -3 to 3
- decode_node_out: bfloat16 [512, 512], replicated, may hold values from -0.25 to 0.25
- decode_node_gain: float32 [512], replicated, may hold values from 0.5 to 1.5
Outputs:
- mesh_out: bfloat16 [131072, 512], P(('member', 'region')), parts along dimension 0
- grid_out: bfloat16 [98304, 512], P(('member', 'region')), parts along dimension 0
The draws below stay inside these ranges and needn't reach their ends.
There are 4 independent parts, one for each index of `member`. The reference program is written for one: setup_inputs(seed, part) draws one part's arguments, and reference() takes and returns one part's arrays. A program takes and returns all parts, laid end to end along the dimension named above; an argument that names none is the same for every part. Nothing has to cross between parts.
Inputs may be any that keep to these rules, and one draw needn't show every extreme that they name: The first mesh_live[d] slots of region d are live and the rest are padding; in every draw some region has all 2048 slots live. `mesh_sender`: a value below 512 names a node of the region itself; 512 + s * 8 + k names the k-th node that the region reads from region s; most slots name the region's own nodes, most remote reads come from its four neighbours, and a few reach any region. `grid_sender`: a value below 512 names a node of the region's mesh_out; 512 + j * 8 + k names the k-th node read from its j-th neighbour; most edges name the region's own nodes.
All inputs are finite; a program needn't handle non-finite values.
Results may differ from the reference program's by a relative error of at most 0.007.
Values may be sent and summed in bfloat16 or wider, within the bound.
No kernel may reach another device: no remote copies, remote signals or barrier semaphores. Data moves between devices by JAX's collectives and lax.ppermute only.
A program may use at most 64 MiB of HBM per device.

```python
import jax
import jax.numpy as jnp
from jax import lax

LATENT = 512
MESH_DEV = 512
GRID_DEV = 384
BOUNDARY = 32
PAIR = 8
REGIONS = 64
EDGES = 2048
GRID_EDGES = 1152
MESH_NODES = 32768
GRID_NODES = 24576


def draw_mesh_live(key, part):
    first_key, second_key = jax.random.split(jax.random.fold_in(key, 11))
    counts = jax.random.randint(first_key, (REGIONS,), EDGES // 4, EDGES + 1)
    fullest = jax.random.randint(second_key, (), 0, REGIONS)
    return jnp.where(jnp.arange(REGIONS) == fullest, EDGES, counts).astype(jnp.int32)


def draw_mesh_sender(key, part):
    keys = jax.random.split(jax.random.fold_in(key, 23), 5)
    shape = (REGIONS, EDGES)
    kind = jax.random.randint(keys[0], shape, 0, 10)
    local = jax.random.randint(keys[1], shape, 0, MESH_DEV)
    offsets = jnp.array([-2, -1, 1, 2], dtype=jnp.int32)
    near = offsets[jax.random.randint(keys[2], shape, 0, 4)]
    region = jnp.arange(REGIONS, dtype=jnp.int32)[:, None]
    near_source = (region + near) % REGIONS
    far_source = jax.random.randint(keys[3], shape, 0, REGIONS)
    slot = jax.random.randint(keys[4], shape, 0, PAIR)
    source = jnp.where(kind < 9, near_source, far_source)
    remote = MESH_DEV + source * PAIR + slot
    return jnp.where(kind < 6, local, remote).astype(jnp.int32)


def draw_grid_sender(key, part):
    keys = jax.random.split(jax.random.fold_in(key, 37), 3)
    shape = (REGIONS, GRID_EDGES)
    kind = jax.random.randint(keys[0], shape, 0, 5)
    local = jax.random.randint(keys[1], shape, 0, MESH_DEV)
    remote = MESH_DEV + jax.random.randint(keys[2], shape, 0, 4 * PAIR)
    return jnp.where(kind < 4, local, remote).astype(jnp.int32)


def place_ends(result, rng, smallest, top_value):
    longest = result.shape.index(max(result.shape))
    spots = []
    for shift in (0, 1):
        where = [jax.random.randint(jax.random.fold_in(rng, axis), (), 0, length) for axis, length in enumerate(result.shape)]
        where[longest] = (where[longest] + shift) % result.shape[longest]
        spots.append(tuple(where))
    return result.at[spots[0]].set(smallest).at[spots[1]].set(top_value)


def shard_levels(key, shape, shards, low, top_value):
    def one(axis_at, shards_of):
        heights = jax.random.uniform(jax.random.fold_in(jax.random.fold_in(key, 6), axis_at), (shards_of,), jnp.float32, low / len(shards), top_value / len(shards))
        return jnp.repeat(jnp.exp(heights), shape[axis_at] // shards_of).reshape((-1,) + (1,) * (len(shape) - axis_at - 1))

    level = one(*shards[0])
    for cut in shards[1:]:
        level = level * one(*cut)
    return level


def gaussian(rng, extent, deviation, most, cuts=(), held_as=jnp.bfloat16):
    values = deviation * jax.random.normal(rng, extent, jnp.float32)
    if cuts:
        values = values * shard_levels(rng, extent, cuts, -0.22, 0.18)
    return jnp.clip(values, -most, most).astype(held_as)


def setup_inputs(seed: int = 0, part: int = 0) -> dict:
    key_list = jax.random.split(jax.random.key(seed), 29)
    own_keys = jax.random.split(jax.random.fold_in(key_list[28], part), 29)
    mesh_nodes = gaussian(own_keys[0], (MESH_NODES, LATENT), 1.0, 6.0, ((0, 64),))
    mesh_edges = gaussian(key_list[1], (REGIONS * EDGES, LATENT), 1.0, 6.0, ((0, 64),))
    grid_nodes = gaussian(own_keys[2], (GRID_NODES, LATENT), 1.0, 6.0, ((0, 64),))
    grid_edges = gaussian(key_list[3], (REGIONS * GRID_EDGES, LATENT), 1.0, 6.0, ((0, 64),))
    boundary = place_ends(jax.random.randint(key_list[4], (REGIONS, BOUNDARY), 0, MESH_DEV), jax.random.fold_in(key_list[4], 1), 0, MESH_DEV - 1).astype(jnp.int32)
    mesh_need = place_ends(jax.random.randint(key_list[5], (REGIONS, REGIONS, PAIR), 0, BOUNDARY), jax.random.fold_in(key_list[5], 1), 0, BOUNDARY - 1).astype(jnp.int32)
    mesh_sender = draw_mesh_sender(jax.random.fold_in(key_list[28], 71), part)
    mesh_receiver = place_ends(jax.random.randint(key_list[7], (REGIONS, EDGES), 0, MESH_DEV), jax.random.fold_in(key_list[7], 1), 0, MESH_DEV - 1).astype(jnp.int32)
    mesh_live = draw_mesh_live(jax.random.fold_in(key_list[28], 71), part)
    grid_need = place_ends(jax.random.randint(key_list[9], (REGIONS, 4, PAIR), 0, BOUNDARY), jax.random.fold_in(key_list[9], 1), 0, BOUNDARY - 1).astype(jnp.int32)
    grid_sender = draw_grid_sender(jax.random.fold_in(key_list[28], 71), part)
    grid_receiver = place_ends(jax.random.randint(key_list[11], (REGIONS, GRID_EDGES), 0, GRID_DEV), jax.random.fold_in(key_list[11], 1), 0, GRID_DEV - 1).astype(jnp.int32)
    process_edge_in = gaussian(key_list[12], (3 * LATENT, LATENT), (3 * LATENT) ** -0.5, 0.15625)
    process_edge_bias = gaussian(key_list[13], (LATENT,), 0.5, 3.0, (), jnp.float32)
    process_edge_out = gaussian(key_list[14], (LATENT, LATENT), LATENT ** -0.5, 0.25)
    process_edge_gain = jnp.clip(1.0 + 0.1 * jax.random.normal(key_list[15], (LATENT,), jnp.float32), 0.5, 1.5)
    process_node_in = gaussian(key_list[16], (2 * LATENT, LATENT), (2 * LATENT) ** -0.5, 0.1875)
    process_node_bias = gaussian(key_list[17], (LATENT,), 0.5, 3.0, (), jnp.float32)
    process_node_out = gaussian(key_list[18], (LATENT, LATENT), LATENT ** -0.5, 0.25)
    process_node_gain = jnp.clip(1.0 + 0.1 * jax.random.normal(key_list[19], (LATENT,), jnp.float32), 0.5, 1.5)
    decode_edge_in = gaussian(key_list[20], (3 * LATENT, LATENT), (3 * LATENT) ** -0.5, 0.15625)
    decode_edge_bias = gaussian(key_list[21], (LATENT,), 0.5, 3.0, (), jnp.float32)
    decode_edge_out = gaussian(key_list[22], (LATENT, LATENT), LATENT ** -0.5, 0.25)
    decode_edge_gain = jnp.clip(1.0 + 0.1 * jax.random.normal(key_list[23], (LATENT,), jnp.float32), 0.5, 1.5)
    decode_node_in = gaussian(key_list[24], (2 * LATENT, LATENT), (2 * LATENT) ** -0.5, 0.1875)
    decode_node_bias = gaussian(key_list[25], (LATENT,), 0.5, 3.0, (), jnp.float32)
    decode_node_out = gaussian(key_list[26], (LATENT, LATENT), LATENT ** -0.5, 0.25)
    decode_node_gain = jnp.clip(1.0 + 0.1 * jax.random.normal(key_list[27], (LATENT,), jnp.float32), 0.5, 1.5)
    return dict(mesh_nodes=mesh_nodes, mesh_edges=mesh_edges, grid_nodes=grid_nodes, grid_edges=grid_edges, boundary=boundary, mesh_need=mesh_need, mesh_sender=mesh_sender, mesh_receiver=mesh_receiver, mesh_live=mesh_live, grid_need=grid_need, grid_sender=grid_sender, grid_receiver=grid_receiver, process_edge_in=process_edge_in, process_edge_bias=process_edge_bias, process_edge_out=process_edge_out, process_edge_gain=process_edge_gain, process_node_in=process_node_in, process_node_bias=process_node_bias, process_node_out=process_node_out, process_node_gain=process_node_gain, decode_edge_in=decode_edge_in, decode_edge_bias=decode_edge_bias, decode_edge_out=decode_edge_out, decode_edge_gain=decode_edge_gain, decode_node_in=decode_node_in, decode_node_bias=decode_node_bias, decode_node_out=decode_node_out, decode_node_gain=decode_node_gain)


def network(inputs, w_in, bias, w_out, gain):
    pre_act = jnp.dot(inputs, w_in, preferred_element_type=jnp.float32) + bias
    hidden = jax.nn.silu(pre_act).astype(jnp.bfloat16)
    projected = jnp.dot(hidden, w_out, preferred_element_type=jnp.float32)
    centred = projected - lax.optimization_barrier(jnp.mean(projected, axis=-1, keepdims=True))
    spread = lax.optimization_barrier(jnp.mean(centred * centred, axis=-1, keepdims=True))
    return centred * lax.rsqrt(spread + 0.25) * gain

def halo_for(node_blocks, boundary, need, region):
    chosen = jnp.take_along_axis(boundary, need[region], axis=1)
    remote = node_blocks[jnp.arange(REGIONS, dtype=jnp.int32)[:, None], chosen]
    return jnp.concatenate([node_blocks[region], remote.reshape(-1, LATENT)], axis=0)

def neighbour_halo(node_blocks, boundary, need, region):
    pieces = [node_blocks[region]]
    for slot, offset in enumerate((-2, -1, 1, 2)):
        source = ((region + offset) % REGIONS).astype(jnp.int32)
        chosen = boundary[source][need[region, slot]]
        pieces.append(node_blocks[source][chosen])
    return jnp.concatenate(pieces, axis=0)

def reference(mesh_nodes, mesh_edges, grid_nodes, grid_edges, boundary, mesh_need, mesh_sender, mesh_receiver, mesh_live, grid_need, grid_sender, grid_receiver, process_edge_in, process_edge_bias, process_edge_out, process_edge_gain, process_node_in, process_node_bias, process_node_out, process_node_gain, decode_edge_in, decode_edge_bias, decode_edge_out, decode_edge_gain, decode_node_in, decode_node_bias, decode_node_out, decode_node_gain):
    mesh_blocks = mesh_nodes.reshape(REGIONS, MESH_DEV, LATENT)
    edge_blocks = mesh_edges.reshape(REGIONS, EDGES, LATENT)
    grid_blocks = grid_nodes.reshape(REGIONS, GRID_DEV, LATENT)
    grid_edge_blocks = grid_edges.reshape(REGIONS, GRID_EDGES, LATENT)

    def mesh_region(region):
        halo_rows = halo_for(mesh_blocks, boundary, mesh_need, region)
        own_rows = mesh_blocks[region]
        edge_rows = edge_blocks[region]
        inputs = jnp.concatenate([halo_rows[mesh_sender[region]], own_rows[mesh_receiver[region]], edge_rows], axis=1)
        message = edge_rows.astype(jnp.float32) + network(inputs, process_edge_in, process_edge_bias, process_edge_out, process_edge_gain)
        live_slots = jnp.arange(EDGES, dtype=jnp.int32) < mesh_live[region]
        message = jnp.where(live_slots[:, None], message, 0.0).astype(jnp.bfloat16)
        summed = jax.ops.segment_sum(message.astype(jnp.float32), mesh_receiver[region], num_segments=MESH_DEV).astype(jnp.bfloat16)
        update = network(jnp.concatenate([own_rows, summed], axis=1), process_node_in, process_node_bias, process_node_out, process_node_gain)
        return (own_rows.astype(jnp.float32) + update).astype(jnp.bfloat16)
    mesh_out_blocks = lax.map(mesh_region, jnp.arange(REGIONS, dtype=jnp.int32))

    def grid_region(region):
        halo_rows = neighbour_halo(mesh_out_blocks, boundary, grid_need, region)
        own_rows = grid_blocks[region]
        edge_rows = grid_edge_blocks[region]
        inputs = jnp.concatenate([halo_rows[grid_sender[region]], own_rows[grid_receiver[region]], edge_rows], axis=1)
        message = (edge_rows.astype(jnp.float32) + network(inputs, decode_edge_in, decode_edge_bias, decode_edge_out, decode_edge_gain)).astype(jnp.bfloat16)
        summed = jax.ops.segment_sum(message.astype(jnp.float32), grid_receiver[region], num_segments=GRID_DEV).astype(jnp.bfloat16)
        update = network(jnp.concatenate([own_rows, summed], axis=1), decode_node_in, decode_node_bias, decode_node_out, decode_node_gain)
        return (own_rows.astype(jnp.float32) + update).astype(jnp.bfloat16)
    grid_out_blocks = lax.map(grid_region, jnp.arange(REGIONS, dtype=jnp.int32))
    return (mesh_out_blocks.reshape(-1, LATENT), grid_out_blocks.reshape(-1, LATENT))
```

```python
import functools

import jax
import jax.numpy as jnp
from jax import lax
from jax.experimental import pallas as pl
from jax.experimental.pallas import tpu as pltpu
from jax.sharding import Mesh
from jax.sharding import PartitionSpec as P

REGION = ("z", "core")
MEMBER_REGION = ("member", "z", "core")
BF = jnp.bfloat16
F32 = jnp.float32
I32 = jnp.int32
SEED = 11
STEPS = 5
BLOCK = 512
GRID_BLOCK = 384
LIMIT = 28 * 2**20


def iota(shape, dim):
    return lax.broadcasted_iota(I32, shape, dim)


def ones_where(mask):
    return jnp.where(mask, 1.0, 0.0).astype(BF)


def dot(a, b):
    return jnp.dot(a, b, preferred_element_type=F32)


def dot_t(a, b):
    return lax.dot_general(a, b, (((0,), (0,)), ((), ())), preferred_element_type=F32)


def columns(rows):
    k = rows.shape[0]
    eye = iota((128, 128), 0) == iota((128, 128), 1)
    return [
        jnp.sum(jnp.where(eye, jnp.broadcast_to(rows[j : j + 1, :], (128, 128)), 0), axis=1, keepdims=True)
        for j in range(k)
    ]


def rows_hot(rows, count):
    return jnp.concatenate([ones_where(iota((128, count), 1) == c) for c in columns(rows)], axis=0)


def silu(x):
    return x * (0.5 + 0.5 * jnp.tanh(0.5 * x))


def finish(pre, bias, w_out, gain):
    hidden = silu(pre + bias).astype(BF)
    y = dot(hidden, w_out)
    y = y - jnp.mean(y, axis=1, keepdims=True)
    spread = jnp.mean(y * y, axis=1, keepdims=True)
    return y * lax.rsqrt(spread + 0.25) * gain


def whole(shape):
    return pl.BlockSpec(shape, lambda *_: (0,) * len(shape))


def call(body, grid, ins, outs, scratch=(), flops=0, nbytes=0):
    return pl.pallas_call(
        body,
        grid=grid,
        in_specs=[s for _, s in ins],
        out_specs=[s for _, _, s in outs],
        out_shape=[jax.ShapeDtypeStruct(s, d) for s, d, _ in outs],
        scratch_shapes=list(scratch),
        compiler_params=pltpu.CompilerParams(vmem_limit_bytes=LIMIT),
        cost_estimate=pl.CostEstimate(flops=flops, bytes_accessed=nbytes, transcendentals=0),
    )(*[a for a, _ in ins])


def publish_body(boundary, nodes, out):
    hot = ones_where(iota((nodes.shape[0], boundary.shape[1]), 0) == boundary[...])
    out[...] = dot_t(hot, nodes[...]).astype(BF)


def before_body(sender, receiver, nodes, w_in, edges, out, table_s, table_r):
    n, f = nodes.shape

    @pl.when(pl.program_id(0) == 0)
    def _():
        table_s[...] = dot(nodes[...], w_in[0:f, :]).astype(BF)
        table_r[...] = dot(nodes[...], w_in[f : 2 * f, :]).astype(BF)

    total = dot(edges[...], w_in[2 * f : 3 * f, :])
    total += dot(rows_hot(sender[0], n), table_s[...])
    total += dot(rows_hot(receiver[0], n), table_r[...])
    out[...] = total


def grid_before_body(receiver, nodes, w_in, edges, out, table_r):
    n, f = nodes.shape

    @pl.when(pl.program_id(0) == 0)
    def _():
        table_r[...] = dot(nodes[...], w_in[f : 2 * f, :]).astype(BF)

    out[...] = dot(edges[...], w_in[2 * f : 3 * f, :]) + dot(rows_hot(receiver[0], n), table_r[...])


def block_of(offset, chips):
    bases = (0, SEED, -SEED)
    for k in range(STEPS + 1):
        for j, b in enumerate(bases):
            if (k + b) % chips == offset:
                return 0, 3 * k + j
            if k and (-k - b) % chips == offset:
                return 1, 3 * (k - 1) + j
    raise ValueError(offset)


def remote_body(chips, place, need, w_s, own, other, out):
    z, c = place[0], place[1]
    regions, pair = need.shape
    total = regions * pair
    offered = own.shape[0] // (6 * (STEPS + 1))
    r = iota((total, regions), 0)
    step = r // (2 * pair)
    half = (r // pair) % 2
    sign = 2 * c - 1
    chip = (z + sign * step + chips) % chips
    core = jnp.where(half == 1, 1 - c, c)
    hot = ones_where(iota((total, regions), 1) == 2 * chip + core)
    wanted = dot(hot, need[...].astype(F32).astype(BF))
    lane = iota((total, pair), 1) == iota((total, pair), 0) % pair
    column = jnp.sum(jnp.where(lane, wanted, 0.0), axis=1, keepdims=True).astype(I32)
    width = 2 * offered
    pieces = []
    for offset in range(chips):
        which, b = block_of(offset, chips)
        source = own if which == 0 else other
        rows = column[offset * 2 * pair : (offset + 1) * 2 * pair, :]
        own_half = iota((2 * pair, width), 0) // pair
        at = (own_half if (which == 0) == (b % 3 < 2) else 1 - own_half) * offered + rows
        pieces.append(dot(ones_where(iota((2 * pair, width), 1) == at), source[b * width : (b + 1) * width, :]))
    chosen = jnp.concatenate(pieces, axis=0).astype(BF)
    out[...] = dot(chosen, w_s[...]).astype(BF)


def mesh_body(chips, pair, place, live, sender, receiver, receiver_row, boundary, nodes, table, edges, before, bias, w_out, gain,
              node_in, node_bias, node_out, node_gain, result, published, totals):
    z, c = place[0], place[1]
    n, f = nodes.shape
    step = pl.program_id(0)
    rows = edges.shape[0]
    far = sender[0] - n
    sign = 2 * c - 1
    region = far // pair
    offset = (sign * (region // 2 - z) + 2 * chips) % chips
    half = jnp.where(region % 2 == c, 0, 1)
    place_of = jnp.where(far >= 0, offset * 2 * pair + half * pair + far % pair, -1)
    pre = before[...] + dot(rows_hot(place_of, table.shape[0]), table[...])
    update = finish(pre, bias[...], w_out[...], gain[...])
    message = (edges[...].astype(F32) + update).astype(BF)
    position = step * rows + iota((1, rows), 1)
    target = jnp.where(position < live[0], receiver_row[0], -1)
    part = dot(ones_where(iota((n, rows), 0) == target), message)

    @pl.when(step == 0)
    def _():
        totals[...] = part

    @pl.when(step > 0)
    def _():
        totals[...] += part

    @pl.when(step == pl.num_programs(0) - 1)
    def _():
        summed = totals[...].astype(BF)
        pre = dot(nodes[...], node_in[0:f, :]) + dot(summed, node_in[f : 2 * f, :])
        update = finish(pre, node_bias[...], node_out[...], node_gain[...])
        value = (nodes[...].astype(F32) + update).astype(BF)
        result[...] = value
        hot = ones_where(iota((n, boundary.shape[1]), 0) == boundary[...])
        published[...] = dot_t(hot, value).astype(BF)


def grid_local_body(sender, mesh_out, w_s, before, out, table):
    n = mesh_out.shape[0]

    @pl.when(pl.program_id(0) == 0)
    def _():
        table[...] = dot(mesh_out[...], w_s[...]).astype(BF)

    out[...] = before[...] + dot(rows_hot(sender[0], n), table[...])


def grid_body(mesh_count, pair, sender, receiver_row, wanted, a, b, c, d, w_s, nodes, edges, before, bias, w_out, gain,
              node_in, node_bias, node_out, node_gain, result, totals, table):
    n, f = nodes.shape
    step = pl.program_id(0)
    rows = edges.shape[0]

    @pl.when(step == 0)
    def _():
        pieces = []
        for j, block in enumerate((a, b, c, d)):
            hot = ones_where(iota((block.shape[0], pair), 0) == wanted[j : j + 1, :])
            pieces.append(dot_t(hot, block[...]))
        chosen = jnp.concatenate(pieces, axis=0).astype(BF)
        table[...] = dot(chosen, w_s[...]).astype(BF)

    pre = before[...] + dot(rows_hot(sender[0] - mesh_count, table.shape[0]), table[...])
    update = finish(pre, bias[...], w_out[...], gain[...])
    message = (edges[...].astype(F32) + update).astype(BF)
    part = dot(ones_where(iota((n, rows), 0) == receiver_row[0]), message)

    @pl.when(step == 0)
    def _():
        totals[...] = part

    @pl.when(step > 0)
    def _():
        totals[...] += part

    @pl.when(step == pl.num_programs(0) - 1)
    def _():
        summed = totals[...].astype(BF)
        pre = dot(nodes[...], node_in[0:f, :]) + dot(summed, node_in[f : 2 * f, :])
        update = finish(pre, node_bias[...], node_out[...], node_gain[...])
        result[...] = (nodes[...].astype(F32) + update).astype(BF)


def tie(*values):
    return lax.optimization_barrier(values)


def local(
    mesh_nodes,
    mesh_edges,
    grid_nodes,
    grid_edges,
    boundary,
    mesh_need,
    mesh_sender,
    mesh_receiver,
    mesh_live,
    grid_need,
    grid_sender,
    grid_receiver,
    process_edge_in,
    process_edge_bias,
    process_edge_out,
    process_edge_gain,
    process_node_in,
    process_node_bias,
    process_node_out,
    process_node_gain,
    decode_edge_in,
    decode_edge_bias,
    decode_edge_out,
    decode_edge_gain,
    decode_node_in,
    decode_node_bias,
    decode_node_out,
    decode_node_gain,
):
    chips = lax.axis_size("z")
    regions = 2 * chips
    place = jnp.stack([lax.axis_index("z"), lax.axis_index("core")]).astype(I32)
    n, f = mesh_nodes.shape
    edges = mesh_edges.shape[0]
    grid_n = grid_nodes.shape[0]
    grid_e = grid_edges.shape[0]
    offered = boundary.shape[1]
    pair = mesh_need.shape[2]
    smem = pl.BlockSpec(memory_space=pltpu.SMEM)
    row = lambda v: v.reshape(1, -1)
    mesh_steps = edges // BLOCK
    grid_steps = grid_e // GRID_BLOCK
    as_blocks = lambda v, b: v.reshape(-1, b // 128, 128)
    as_rows = lambda v, b: v.reshape(-1, 1, b)
    idx_spec = lambda b: pl.BlockSpec((1, b // 128, 128), lambda i: (i, 0, 0))
    row_spec = lambda b: pl.BlockSpec((1, 1, b), lambda i: (i, 0, 0))
    tile = lambda b: pl.BlockSpec((b, f), lambda i: (i, 0))
    full = lambda v: (v, whole(v.shape))

    def along(steps):
        pairs = []
        for z in range(chips):
            pairs.append((2 * z, 2 * ((z + steps) % chips)))
            pairs.append((2 * z + 1, 2 * ((z - steps) % chips) + 1))
        return pairs

    def shift(v, steps):
        return lax.ppermute(v, REGION, along(steps))

    def swap(v):
        return lax.ppermute(v, "core", [(0, 1), (1, 0)])

    (own,) = call(publish_body, (1,), [full(boundary), full(mesh_nodes)], [((offered, f), BF, whole((offered, f)))],
                  flops=2 * offered * n * f, nbytes=2 * n * f)
    both = jnp.concatenate([own, swap(own)], axis=0)
    seed = shift(both, SEED)
    edges_in, _ = tie(mesh_edges, own)
    (before,) = call(
        before_body, (mesh_steps,),
        [(as_blocks(mesh_sender, BLOCK), idx_spec(BLOCK)), (as_blocks(mesh_receiver, BLOCK), idx_spec(BLOCK)), full(mesh_nodes),
         full(process_edge_in), (edges_in, tile(BLOCK))],
        [((edges, f), F32, tile(BLOCK))],
        [pltpu.VMEM((n, f), BF), pltpu.VMEM((n, f), BF)],
        flops=2 * f * f * (edges * 3 + 2 * n), nbytes=6 * edges * f,
    )
    seed, before = tie(seed, before)
    seed_other = swap(seed)
    current = jnp.concatenate([both, seed, seed_other], axis=0)
    arrived = [current]
    grid_in, _ = tie(grid_edges, current)
    (grid_before,) = call(
        grid_before_body, (grid_steps,),
        [(as_blocks(grid_receiver, GRID_BLOCK), idx_spec(GRID_BLOCK)), full(grid_nodes), full(decode_edge_in),
         (grid_in, tile(GRID_BLOCK))],
        [((grid_e, f), F32, tile(GRID_BLOCK))],
        [pltpu.VMEM((grid_n, f), BF)],
        flops=2 * f * f * (grid_e * 2 + grid_n), nbytes=6 * grid_e * f,
    )
    for k in range(STEPS):
        current = shift(current, 1)
        if k == 0:
            current, grid_before = tie(current, grid_before)
        arrived.append(current)
    own_side = jnp.concatenate(arrived, axis=0)
    other_side = swap(own_side[arrived[0].shape[0] :])
    (table,) = call(
        functools.partial(remote_body, chips), (1,),
        [(place, smem), full(mesh_need[0]), (process_edge_in, whole((f, f))), full(own_side), full(other_side)],
        [((regions * pair, f), BF, whole((regions * pair, f)))],
        flops=2 * f * f * n, nbytes=2 * 2112 * f,
    )
    mesh_out, published = call(
        functools.partial(mesh_body, chips, pair), (mesh_steps,),
        [(place, smem), (mesh_live, smem), (as_blocks(mesh_sender, BLOCK), idx_spec(BLOCK)),
         (as_blocks(mesh_receiver, BLOCK), idx_spec(BLOCK)), (as_rows(mesh_receiver, BLOCK), row_spec(BLOCK)), full(boundary),
         full(mesh_nodes), full(table), (mesh_edges, tile(BLOCK)), (before, tile(BLOCK)), full(row(process_edge_bias)),
         full(process_edge_out), full(row(process_edge_gain)), full(process_node_in), full(row(process_node_bias)),
         full(process_node_out), full(row(process_node_gain))],
        [((n, f), BF, whole((n, f))), ((offered, f), BF, whole((offered, f)))],
        [pltpu.VMEM((n, f), F32)],
        flops=2 * f * f * (edges * 3 + 3 * n), nbytes=6 * edges * f,
    )
    pieces = []
    for offset in (-2, -1, 1, 2):
        pieces.append(lax.ppermute(published, REGION, [(s, (s - offset) % regions) for s in range(regions)]))
    (grid_local,) = call(
        grid_local_body, (grid_steps,),
        [(as_blocks(grid_sender, GRID_BLOCK), idx_spec(GRID_BLOCK)), full(mesh_out), (decode_edge_in, whole((f, f))),
         (grid_before, tile(GRID_BLOCK))],
        [((grid_e, f), F32, tile(GRID_BLOCK))],
        [pltpu.VMEM((n, f), BF)],
        flops=2 * f * f * (grid_e + n), nbytes=8 * grid_e * f,
    )
    (grid_out,) = call(
        functools.partial(grid_body, n, pair), (grid_steps,),
        [(as_blocks(grid_sender, GRID_BLOCK), idx_spec(GRID_BLOCK)), (as_rows(grid_receiver, GRID_BLOCK), row_spec(GRID_BLOCK)),
         full(grid_need[0]), full(pieces[0]), full(pieces[1]), full(pieces[2]), full(pieces[3]),
         (decode_edge_in, whole((f, f))), full(grid_nodes), (grid_edges, tile(GRID_BLOCK)), (grid_local, tile(GRID_BLOCK)),
         full(row(decode_edge_bias)), full(decode_edge_out), full(row(decode_edge_gain)), full(decode_node_in),
         full(row(decode_node_bias)), full(decode_node_out), full(row(decode_node_gain))],
        [((grid_n, f), BF, whole((grid_n, f)))],
        [pltpu.VMEM((grid_n, f), F32), pltpu.VMEM((4 * pair, f), BF)],
        flops=2 * f * f * (grid_e * 2 + 3 * grid_n), nbytes=6 * grid_e * f,
    )
    return (mesh_out, grid_out)


def solution(mesh):
    cores = 2
    finer = Mesh(
        mesh.devices.reshape(mesh.shape["member"], mesh.shape["region"] // cores, cores), ("member", "z", "core")
    )
    in_specs = (
        P(MEMBER_REGION, None),
        P(REGION, None),
        P(MEMBER_REGION, None),
        P(REGION, None),
        P(REGION, None),
        P(REGION, None, None),
        P(REGION, None),
        P(REGION, None),
        P(REGION),
        P(REGION, None, None),
        P(REGION, None),
        P(REGION, None),
    ) + (P(),) * 16
    out_specs = (P(MEMBER_REGION, None), P(MEMBER_REGION, None))
    return jax.shard_map(local, mesh=finer, in_specs=in_specs, out_specs=out_specs, check_vma=False)
```

```python
import functools

import jax
import jax.numpy as jnp
from jax import lax
from jax.experimental import pallas as pl
from jax.experimental.pallas import tpu as pltpu
from jax.sharding import Mesh
from jax.sharding import PartitionSpec as P

REGION = ("z", "core")
MEMBER_REGION = ("member", "z", "core")
BF = jnp.bfloat16
F32 = jnp.float32
I32 = jnp.int32
HBM = pltpu.MemorySpace.HBM
SEED = 12
LEAD = 3
STEPS = 4
BLOCK = 512
GRID_BLOCK = 384
LIMIT = 36 * 2**20


def iota(shape, dim):
    return lax.broadcasted_iota(I32, shape, dim)


def ones_where(mask):
    return jnp.where(mask, 1.0, 0.0).astype(BF)


def dot(a, b):
    return jnp.dot(a, b, preferred_element_type=F32)


def dot_t(a, b):
    return lax.dot_general(a, b, (((0,), (0,)), ((), ())), preferred_element_type=F32)


def columns(rows):
    lines = [rows[i : i + 1, j : j + 128] for i in range(rows.shape[0]) for j in range(0, rows.shape[1], 128)]
    eye = iota((128, 128), 0) == iota((128, 128), 1)
    return [jnp.sum(jnp.where(eye, jnp.broadcast_to(line, (128, 128)), 0), axis=1, keepdims=True) for line in lines]


def rows_hot(rows, count):
    return jnp.concatenate([ones_where(iota((128, count), 1) == c) for c in columns(rows)], axis=0)


def silu(x):
    return x * (0.5 + 0.5 * jnp.tanh(0.5 * x))


def finish(pre, bias, w_out, gain):
    hidden = silu(pre + bias).astype(BF)
    y = dot(hidden, w_out)
    y = y - jnp.mean(y, axis=1, keepdims=True)
    spread = jnp.mean(y * y, axis=1, keepdims=True)
    return y * lax.rsqrt(spread + 0.25) * gain


def whole(shape):
    return pl.BlockSpec(shape, lambda *_: (0,) * len(shape))


def call(body, grid, ins, outs, scratch=(), flops=0, nbytes=0):
    place = lambda a, s, *near: a if near or s.memory_space not in (None, HBM) else pltpu.with_memory_space_constraint(a, HBM)
    result = lambda s, d, p, *far: HBM(s, d) if far or p.memory_space == HBM else jax.ShapeDtypeStruct(s, d)
    return pl.pallas_call(
        body,
        grid=grid,
        in_specs=[i[1] for i in ins],
        out_specs=[o[2] for o in outs],
        out_shape=[result(*o) for o in outs],
        scratch_shapes=list(scratch),
        compiler_params=pltpu.CompilerParams(vmem_limit_bytes=LIMIT),
        cost_estimate=pl.CostEstimate(flops=flops, bytes_accessed=nbytes, transcendentals=0),
    )(*[place(*i) for i in ins])


def publish_body(boundary_hbm, nodes_hbm, out, boundary, nodes, sems):
    copies = [pltpu.make_async_copy(boundary_hbm, boundary, sems.at[0]), pltpu.make_async_copy(nodes_hbm, nodes, sems.at[1])]
    for copy in copies:
        copy.start()
    for copy in copies:
        copy.wait()
    hot = ones_where(iota((nodes.shape[0], boundary.shape[1]), 0) == boundary[...])
    out[...] = dot_t(hot, nodes[...]).astype(BF)


def before_body(sender, receiver, nodes, w_in, edges, ready, out, table_r, table_s):
    n, f = nodes.shape

    @pl.when(pl.program_id(0) == 0)
    def _():
        table_s[...] = dot(nodes[...], w_in[0:f, :]).astype(BF)
        table_r[...] = dot(nodes[...], w_in[f : 2 * f, :]).astype(BF)

    total = dot(edges[...], w_in[2 * f : 3 * f, :])
    total += dot(rows_hot(sender[0], n), table_s[...])
    total += dot(rows_hot(receiver[0], n), table_r[...])
    out[...] = total


def grid_before_body(receiver, nodes, w_in, edges, ready, out, table_r):
    n, f = nodes.shape

    @pl.when(pl.program_id(0) == 0)
    def _():
        table_r[...] = dot(nodes[...], w_in[f : 2 * f, :]).astype(BF)

    out[...] = dot(edges[...], w_in[2 * f : 3 * f, :]) + dot(rows_hot(receiver[0], n), table_r[...])


def pieces_of(chips, offered):
    pair = 2 * offered
    far = [(2, 0), (-2, 1)]
    for step in range(STEPS + 1):
        far += [(LEAD + step, 0), (SEED + step, 0), (step - SEED, 1)]
    far += [(-LEAD, 1)]
    for step in range(1, STEPS + 1):
        far += [(-LEAD - step, 1), (-SEED - step, 1), (SEED - step, 0)]
    table = {}
    for i, (offset, flip) in enumerate(far):
        table.setdefault(offset % chips, (i * pair, flip))
    return table


def relative(sender, n, pair, chips, z, c):
    far = sender - n
    region = far // pair
    sign = 2 * c - 1
    offset = (sign * (region // 2 - z) + 2 * chips) % chips
    half = jnp.where(region % 2 == c, 0, 1)
    return far >= 0, region, offset, half, far % pair


def is_near(offset, chips):
    return (offset <= 1) | (offset == chips - 1)


def main_body(chips, first, place, live, sender, sender_row, receiver_row, need, w_s, both, up, down, edges, before, bias, w_out,
              gain, start, ready, totals, table):
    z, c = place[0], place[1]
    n, _ = totals.shape
    step = pl.program_id(0)
    rows = edges.shape[0]
    pair, regions = need.shape
    offered = both.shape[0] // 2

    @pl.when(step == 0)
    def _():
        totals[...] = start[...]
        r = iota((6 * pair, regions), 0)
        near = r // (2 * pair)
        half = (r // pair) % 2
        moved = jnp.where(near == 2, -1, near)
        chip = (z + (2 * c - 1) * moved + chips) % chips
        region = 2 * chip + jnp.where(half == 1, 1 - c, c)
        wanted = lax.dot_general(ones_where(iota((6 * pair, regions), 1) == region), need[...].astype(F32).astype(BF),
                                 (((1,), (1,)), ((), ())), preferred_element_type=F32)
        lane = iota((6 * pair, pair), 1) == iota((6 * pair, pair), 0) % pair
        column = jnp.sum(jnp.where(lane, wanted, 0.0), axis=1, keepdims=True).astype(I32)
        chosen = []
        for j, (source, flip) in enumerate(((both, 0), (up, 0), (down, 1))):
            own_half = iota((2 * pair, 2 * offered), 0) // pair
            at = (1 - own_half if flip else own_half) * offered + column[j * 2 * pair : (j + 1) * 2 * pair, :]
            chosen.append(dot(ones_where(iota((2 * pair, 2 * offered), 1) == at), source[...]))
        table[...] = dot(jnp.concatenate(chosen, axis=0).astype(BF), w_s[...]).astype(BF)

    remote, _, offset, half, slot = relative(sender[0], n, pair, chips, z, c)
    near = jnp.where(offset == chips - 1, 2, offset)
    place_of = jnp.where(remote & is_near(offset, chips), near * 2 * pair + half * pair + slot, -1)
    pre = before[...] + dot(rows_hot(place_of, 6 * pair), table[...])
    update = finish(pre, bias[...], w_out[...], gain[...])
    message = (edges[...].astype(F32) + update).astype(BF)
    position = (first + step) * rows + iota((1, rows), 1)
    remote, _, offset, _, _ = relative(sender_row[0], n, pair, chips, z, c)
    later = remote & jnp.logical_not(is_near(offset, chips))
    target = jnp.where((position < live[0]) & jnp.logical_not(later), receiver_row[0], -1)
    totals[...] += dot(ones_where(iota((n, rows), 0) == target), message)


def gathered(at, sources, starts):
    out = None
    for source, start in zip(sources, starts):
        hot = ones_where(iota((at.shape[0], source.shape[0]), 1) + start == at)
        part = dot(hot, source[...])
        out = part if out is None else out + part
    return out


def compact_body(chips, offered, starts, place, live, sender, receiver, need, w_in, table_r, edges, *refs):
    sources = refs[: len(starts)]
    outs, count, kept, sems = refs[len(starts) : len(starts) + 5], refs[len(starts) + 5], refs[-6:-1], refs[-1]
    pre, rows, source_rows, at_out, target_out = kept
    z, c = place[0], place[1]
    groups = sender.shape[0]
    n, f = table_r.shape
    pair, regions = need.shape
    where_at = pieces_of(chips, offered)
    send = sender[...]
    remote, _, offset, _, _ = relative(send, n, pair, chips, z, c)
    position = iota((groups, 128), 0) * 128 + iota((groups, 128), 1)
    late = remote & jnp.logical_not(is_near(offset, chips)) & (position < live[0])
    late_bits = ones_where(late)
    within = dot(late_bits, ones_where(iota((128, 128), 0) < iota((128, 128), 1)))
    above = jnp.sum(dot(ones_where(iota((groups, groups), 1) < iota((groups, groups), 0)), late_bits), axis=1, keepdims=True)
    rank = jnp.where(late, (within + above).astype(I32), -1)
    total = jnp.sum(jnp.where(late, 1, 0))
    blocks = (total + 127) // 128
    count[0] = blocks

    def one(block, carry):
        base = pl.multiple_of(block * 128, 128)
        lines = pl.ds(base, 128)
        hot, send_at, receive_at = [], jnp.zeros((128, 128), I32), jnp.zeros((128, 128), I32)
        for g in range(groups):
            match = iota((128, 128), 0) + base == rank[g : g + 1, :]
            hot.append(ones_where(match))
            send_at += jnp.where(match, send[g : g + 1, :] + 1, 0)
            receive_at += jnp.where(match, receiver[g : g + 1, :] + 1, 0)
        edge = dot(jnp.concatenate(hot, axis=1), edges[...]).astype(BF)
        from_ = jnp.sum(send_at, axis=1, keepdims=True) - 1
        to = jnp.sum(receive_at, axis=1, keepdims=True) - 1
        valid, region, offset, half, slot = relative(from_, n, pair, chips, z, c)
        wanted = lax.dot_general(ones_where(iota((128, regions), 1) == region), need[...].astype(F32).astype(BF),
                                 (((1,), (1,)), ((), ())), preferred_element_type=F32)
        chosen = jnp.sum(jnp.where(iota((128, pair), 1) == slot, wanted, 0.0), axis=1, keepdims=True).astype(I32)
        start, flip = jnp.zeros((128, 1), I32), jnp.zeros((128, 1), I32)
        for key, (row, turned) in where_at.items():
            start = jnp.where(offset == key, row, start)
            flip = jnp.where(offset == key, turned, flip)
        at = jnp.where(valid, start + jnp.where(flip == 1, 1 - half, half) * offered + chosen, -1)
        rows[...] = edge
        pre[...] = dot(edge, w_in[2 * f : 3 * f, :]) + dot(ones_where(iota((128, n), 1) == to), table_r[...])
        source_rows[...] = gathered(at, sources, starts).astype(BF)
        at_out[...] = jnp.broadcast_to(at, (128, 128))
        target_out[...] = jnp.broadcast_to(to, (128, 128))
        copies = [pltpu.make_async_copy(v, o.at[lines, :], sems.at[i]) for i, (v, o) in enumerate(zip(kept, outs))]
        for copy in copies:
            copy.start()
        for copy in copies:
            copy.wait()
        return carry

    lax.fori_loop(0, blocks, one, 0)


def far_body(starts, count, nodes, boundary, totals, bias, gain, node_bias, node_gain, *refs):
    k = len(starts)
    sources = refs[:k]
    stored = refs[k : k + 5]
    (w_s_hbm, w_out_hbm, node_in_hbm, node_out_hbm, result, kept_result, published, acc, w_s, w_out, node_in, node_out, sems) = refs[k + 5 : -6]
    kept, late_sems = refs[-6:-1], refs[-1]
    pre, rows, source_rows, at, target = kept
    n, f = nodes.shape
    copies = [
        pltpu.make_async_copy(w_s_hbm.at[pl.ds(0, f), :], w_s, sems.at[0]),
        pltpu.make_async_copy(w_out_hbm, w_out, sems.at[1]),
        pltpu.make_async_copy(node_in_hbm, node_in, sems.at[2]),
        pltpu.make_async_copy(node_out_hbm, node_out, sems.at[3]),
    ]
    for copy in copies:
        copy.start()

    def fetch(block, begin):
        lines = pl.ds(pl.multiple_of(block * 128, 128), 128)
        for i, (v, o) in enumerate(zip(stored, kept)):
            copy = pltpu.make_async_copy(v.at[lines, :], o, late_sems.at[i])
            copy.start() if begin else copy.wait()

    @pl.when(count[0] > 0)
    def _():
        fetch(0, True)

    acc[...] = totals[...]
    copies[0].wait()
    copies[1].wait()

    def one(block, carry):
        fetch(block, False)
        source = (source_rows[...].astype(F32) + gathered(at[...][:, 0:1], sources, starts)).astype(BF)
        update = finish(pre[...] + dot(source, w_s[...]), bias[...], w_out[...], gain[...])
        message = (rows[...].astype(F32) + update).astype(BF)
        eye = iota((128, 128), 0) == iota((128, 128), 1)
        to = jnp.sum(jnp.where(eye, target[...] + 1, 0), axis=0, keepdims=True) - 1
        acc[...] += dot(ones_where(iota((n, 128), 0) == to), message)

        @pl.when(block + 1 < count[0])
        def _():
            fetch(block + 1, True)

        return carry

    lax.fori_loop(0, count[0], one, 0)
    copies[2].wait()
    copies[3].wait()
    pre_node = dot(nodes[...], node_in[0:f, :]) + dot(acc[...].astype(BF), node_in[f : 2 * f, :])
    update = finish(pre_node, node_bias[...], node_out[...], node_gain[...])
    value = (nodes[...].astype(F32) + update).astype(BF)
    result[...] = value
    kept_result[...] = value
    hot = ones_where(iota((n, boundary.shape[1]), 0) == boundary[...])
    published[...] = dot_t(hot, value).astype(BF)


def grid_local_body(sender, mesh_out, w_s, before, out, table):
    n = mesh_out.shape[0]

    @pl.when(pl.program_id(0) == 0)
    def _():
        table[...] = dot(mesh_out[...], w_s[...]).astype(BF)

    out[...] = before[...] + dot(rows_hot(sender[0], n), table[...])


def grid_body(mesh_count, pair, sender, receiver_row, wanted, a, b, c, d, w_s, nodes, edges, before, bias, w_out, gain,
              node_in, node_bias, node_out, node_gain, result, totals, table):
    n, f = nodes.shape
    step = pl.program_id(0)
    rows = edges.shape[0]

    @pl.when(step == 0)
    def _():
        pieces = []
        for j, block in enumerate((a, b, c, d)):
            hot = ones_where(iota((block.shape[0], pair), 0) == wanted[j : j + 1, :])
            pieces.append(dot_t(hot, block[...]))
        chosen = jnp.concatenate(pieces, axis=0).astype(BF)
        table[...] = dot(chosen, w_s[...]).astype(BF)

    pre = before[...] + dot(rows_hot(sender[0] - mesh_count, table.shape[0]), table[...])
    update = finish(pre, bias[...], w_out[...], gain[...])
    message = (edges[...].astype(F32) + update).astype(BF)
    part = dot(ones_where(iota((n, rows), 0) == receiver_row[0]), message)

    @pl.when(step == 0)
    def _():
        totals[...] = part

    @pl.when(step > 0)
    def _():
        totals[...] += part

    @pl.when(step == pl.num_programs(0) - 1)
    def _():
        summed = totals[...].astype(BF)
        pre = dot(nodes[...], node_in[0:f, :]) + dot(summed, node_in[f : 2 * f, :])
        update = finish(pre, node_bias[...], node_out[...], node_gain[...])
        result[...] = (nodes[...].astype(F32) + update).astype(BF)


def local(
    mesh_nodes,
    mesh_edges,
    grid_nodes,
    grid_edges,
    boundary,
    mesh_need,
    mesh_sender,
    mesh_receiver,
    mesh_live,
    grid_need,
    grid_sender,
    grid_receiver,
    process_edge_in,
    process_edge_bias,
    process_edge_out,
    process_edge_gain,
    process_node_in,
    process_node_bias,
    process_node_out,
    process_node_gain,
    decode_edge_in,
    decode_edge_bias,
    decode_edge_out,
    decode_edge_gain,
    decode_node_in,
    decode_node_bias,
    decode_node_out,
    decode_node_gain,
):
    chips = lax.axis_size("z")
    regions = 2 * chips
    place = jnp.stack([lax.axis_index("z"), lax.axis_index("core")]).astype(I32)
    n, f = mesh_nodes.shape
    edges = mesh_edges.shape[0]
    grid_n = grid_nodes.shape[0]
    grid_e = grid_edges.shape[0]
    offered = boundary.shape[1]
    pair = mesh_need.shape[2]
    smem = pl.BlockSpec(memory_space=pltpu.SMEM)
    row = lambda v: v.reshape(1, -1)
    mesh_steps = edges // BLOCK
    grid_steps = grid_e // GRID_BLOCK
    as_blocks = lambda v, b: v.reshape(-1, b // 128, 128)
    as_rows = lambda v, b: v.reshape(-1, 1, b)
    idx_spec = lambda b: pl.BlockSpec((1, b // 128, 128), lambda i: (i, 0, 0))
    row_spec = lambda b: pl.BlockSpec((1, 1, b), lambda i: (i, 0, 0))
    tile = lambda b: pl.BlockSpec((b, f), lambda i: (i, 0))
    full = lambda v: (v, whole(v.shape))
    held = lambda v: (v, whole(v.shape), True)

    def along(steps):
        pairs = []
        for z in range(chips):
            pairs.append((2 * z, 2 * ((z + steps) % chips)))
            pairs.append((2 * z + 1, 2 * ((z - steps) % chips) + 1))
        return pairs

    def shift(v, steps):
        return lax.ppermute(v, REGION, along(steps))

    def swap(v):
        return lax.ppermute(v, "core", [(0, 1), (1, 0)])

    hbm = pl.BlockSpec(memory_space=HBM)
    anywhere = pl.BlockSpec(memory_space=pl.ANY)
    need = jnp.transpose(mesh_need[0])
    send_rows = mesh_sender.reshape(-1, 128)
    receive_rows = mesh_receiver.reshape(-1, 128)

    (own,) = call(publish_body, (1,), [(boundary, hbm), (mesh_nodes, hbm)], [((offered, f), BF, whole((offered, f)))],
                  [pltpu.VMEM((1, offered), I32), pltpu.VMEM((n, f), BF), pltpu.SemaphoreType.DMA((2,))],
                  flops=2 * offered * n * f, nbytes=2 * n * f)
    both = jnp.concatenate([own, swap(own)], axis=0)
    lead = [both]
    lead.append(shift(both, 1))
    seed = shift(both, SEED)
    lead.append(shift(lead[1], 1))
    lead.append(shift(lead[2], 1))
    back = [None]
    for k in range(1, LEAD + 1):
        back.append(swap(lead[k]))
    seed_back = swap(seed)
    before, table_r = call(
        before_body, (mesh_steps,),
        [(as_blocks(mesh_sender, BLOCK), idx_spec(BLOCK)), (as_blocks(mesh_receiver, BLOCK), idx_spec(BLOCK)), full(mesh_nodes),
         full(process_edge_in), (mesh_edges, tile(BLOCK)), (lead[1], anywhere)],
        [((edges, f), F32, tile(BLOCK), True), ((n, f), BF, whole((n, f)))],
        [pltpu.VMEM((n, f), BF)],
        flops=2 * f * f * (edges * 3 + 2 * n), nbytes=6 * edges * f,
    )
    halves = mesh_steps // 2
    totals = jnp.zeros((n, f), F32)
    ready = lead[2]
    current = jnp.concatenate([lead[3], seed, seed_back], axis=0)
    chain, turned = [current], []
    for _ in range(STEPS):
        chain.append(shift(chain[-1], 1))
        turned.append(swap(chain[-1]))
    for part in range(2):
        first = part * halves
        at = lambda spec_rows, rank: pl.BlockSpec((1,) + spec_rows, lambda i: (i + first,) + (0,) * rank)
        moved = pl.BlockSpec((BLOCK, f), lambda i: (i + first, 0))
        (totals,) = call(
            functools.partial(main_body, chips, first), (halves,),
            [(place, smem), (mesh_live, smem), (as_blocks(mesh_sender, BLOCK), at((BLOCK // 128, 128), 2)),
             (as_rows(mesh_sender, BLOCK), at((1, BLOCK), 2)), (as_rows(mesh_receiver, BLOCK), at((1, BLOCK), 2)), full(need),
             (process_edge_in, whole((f, f))), held(lead[0]), held(lead[1]), held(back[1]), (mesh_edges, moved),
             (before, moved), full(row(process_edge_bias)), full(process_edge_out), full(row(process_edge_gain)), full(totals),
             (ready, anywhere)],
            [((n, f), F32, whole((n, f)), True)],
            [pltpu.VMEM((6 * pair, f), BF)],
            flops=2 * f * f * halves * BLOCK * 2, nbytes=6 * halves * BLOCK * f,
        )
        ready = chain[0]
    (grid_before,) = call(
        grid_before_body, (grid_steps,),
        [(as_rows(grid_receiver, GRID_BLOCK), row_spec(GRID_BLOCK)), full(grid_nodes), full(decode_edge_in),
         (grid_edges, tile(GRID_BLOCK)), (chain[1], anywhere)],
        [((grid_e, f), F32, tile(GRID_BLOCK), True)],
        [pltpu.VMEM((grid_n, f), BF)],
        flops=2 * f * f * (grid_e * 2 + grid_n), nbytes=6 * grid_e * f,
    )
    far = [lead[2], back[2]] + chain + [back[3]] + turned
    starts, at_row = [], 0
    for v in far:
        starts.append(at_row)
        at_row += v.shape[0]
    last = [STEPS + 2, len(far) - 2, len(far) - 1]
    early = [i for i in range(len(far)) if i not in last]
    late_buffers = [pltpu.VMEM((128, f), F32), pltpu.VMEM((128, f), BF), pltpu.VMEM((128, f), BF), pltpu.VMEM((128, 128), I32),
                    pltpu.VMEM((128, 128), I32)]
    pre, rows, source_rows, at, target, count = call(
        functools.partial(compact_body, chips, offered, tuple(starts[i] for i in early)), (1,),
        [(place, smem), (mesh_live, smem), full(send_rows), full(receive_rows), full(need), full(process_edge_in), held(table_r),
         full(mesh_edges)] + [held(far[i]) for i in early],
        [((edges, f), F32, hbm), ((edges, f), BF, hbm), ((edges, f), BF, hbm), ((edges, 128), I32, hbm),
         ((edges, 128), I32, hbm), ((1,), I32, smem)],
        late_buffers + [pltpu.SemaphoreType.DMA((5,))],
        flops=2 * f * 128 * (edges + 4 * f), nbytes=2 * edges * f,
    )
    mesh_out, mesh_kept, published = call(
        functools.partial(far_body, tuple(starts[i] for i in last)), (1,),
        [(count, smem), full(mesh_nodes), full(boundary), full(totals), full(row(process_edge_bias)), full(row(process_edge_gain)),
         full(row(process_node_bias)), full(row(process_node_gain))] + [held(far[i]) for i in last]
        + [(v, hbm) for v in (pre, rows, source_rows, at, target)] + [(process_edge_in, hbm), (process_edge_out, hbm), (process_node_in, hbm), (process_node_out, hbm)],
        [((n, f), BF, whole((n, f))), ((n, f), BF, whole((n, f))), ((offered, f), BF, whole((offered, f)))],
        [pltpu.VMEM((n, f), F32), pltpu.VMEM((f, f), BF), pltpu.VMEM((f, f), BF), pltpu.VMEM((2 * f, f), BF), pltpu.VMEM((f, f), BF),
         pltpu.SemaphoreType.DMA((4,))] + late_buffers + [pltpu.SemaphoreType.DMA((5,))],
        flops=2 * f * f * 4 * n, nbytes=8 * n * f,
    )
    pieces = []
    for offset in (-2, -1, 1, 2):
        pieces.append(lax.ppermute(published, REGION, [(s, (s - offset) % regions) for s in range(regions)]))
    (grid_local,) = call(
        grid_local_body, (grid_steps,),
        [(as_rows(grid_sender, GRID_BLOCK), row_spec(GRID_BLOCK)), held(mesh_kept), (decode_edge_in, whole((f, f))),
         (grid_before, tile(GRID_BLOCK))],
        [((grid_e, f), F32, tile(GRID_BLOCK))],
        [pltpu.VMEM((n, f), BF)],
        flops=2 * f * f * (grid_e + n), nbytes=8 * grid_e * f,
    )
    (grid_out,) = call(
        functools.partial(grid_body, n, pair), (grid_steps,),
        [(as_rows(grid_sender, GRID_BLOCK), row_spec(GRID_BLOCK)), (as_rows(grid_receiver, GRID_BLOCK), row_spec(GRID_BLOCK)),
         full(grid_need[0]), held(pieces[0]), held(pieces[1]), held(pieces[2]), held(pieces[3]),
         (decode_edge_in, whole((f, f))), full(grid_nodes), (grid_edges, tile(GRID_BLOCK)), (grid_local, tile(GRID_BLOCK), True),
         full(row(decode_edge_bias)), full(decode_edge_out), full(row(decode_edge_gain)), full(decode_node_in),
         full(row(decode_node_bias)), full(decode_node_out), full(row(decode_node_gain))],
        [((grid_n, f), BF, whole((grid_n, f)))],
        [pltpu.VMEM((grid_n, f), F32), pltpu.VMEM((4 * pair, f), BF)],
        flops=2 * f * f * (grid_e * 2 + 3 * grid_n), nbytes=6 * grid_e * f,
    )
    return (mesh_out, grid_out)


def solution(mesh):
    cores = 2
    finer = Mesh(
        mesh.devices.reshape(mesh.shape["member"], mesh.shape["region"] // cores, cores), ("member", "z", "core")
    )
    in_specs = (
        P(MEMBER_REGION, None),
        P(REGION, None),
        P(MEMBER_REGION, None),
        P(REGION, None),
        P(REGION, None),
        P(REGION, None, None),
        P(REGION, None),
        P(REGION, None),
        P(REGION),
        P(REGION, None, None),
        P(REGION, None),
        P(REGION, None),
    ) + (P(),) * 16
    out_specs = (P(MEMBER_REGION, None), P(MEMBER_REGION, None))

    return jax.shard_map(local, mesh=finer, in_specs=in_specs, out_specs=out_specs, check_vma=False)
```

```python
import functools

import jax
import jax.numpy as jnp
from jax import lax
from jax.experimental import pallas as pl
from jax.experimental.pallas import tpu as pltpu
from jax.sharding import Mesh
from jax.sharding import PartitionSpec as P

REGION = ("z", "core")
MEMBER_REGION = ("member", "z", "core")
BF = jnp.bfloat16
F32 = jnp.float32
I32 = jnp.int32
HBM = pltpu.MemorySpace.HBM
VMEM = pltpu.MemorySpace.VMEM
SEED = 12
LEAD = 3
STEPS = 4
AHEAD_FAR = 6
AHEAD_GRID = 7
BLOCK = 512
GRID_BLOCK = 384
LIMIT = 24 * 2**20


def iota(shape, dim):
    return lax.broadcasted_iota(I32, shape, dim)


def ones_where(mask):
    return jnp.where(mask, 1.0, 0.0).astype(BF)


def dot(a, b):
    return jnp.dot(a, b, preferred_element_type=F32)


def dot_t(a, b):
    return lax.dot_general(a, b, (((0,), (0,)), ((), ())), preferred_element_type=F32)


def columns(rows):
    lines = [rows[i : i + 1, j : j + 128] for i in range(rows.shape[0]) for j in range(0, rows.shape[1], 128)]
    eye = iota((128, 128), 0) == iota((128, 128), 1)
    return [jnp.sum(jnp.where(eye, jnp.broadcast_to(line, (128, 128)), 0), axis=1, keepdims=True) for line in lines]


def rows_hot(rows, count):
    return jnp.concatenate([ones_where(iota((128, count), 1) == c) for c in columns(rows)], axis=0)


def silu(x):
    return x * (0.5 + 0.5 * jnp.tanh(0.5 * x))


def finish(pre, bias, w_out, gain):
    hidden = silu(pre + bias).astype(BF)
    y = dot(hidden, w_out)
    y = y - jnp.mean(y, axis=1, keepdims=True)
    spread = jnp.mean(y * y, axis=1, keepdims=True)
    return y * lax.rsqrt(spread + 0.25) * gain


def whole(shape):
    return pl.BlockSpec(shape, lambda *_: (0,) * len(shape))


def call(body, grid, ins, outs, scratch=(), flops=0, nbytes=0):
    place = lambda a, s, *near: a if near or s.memory_space not in (None, HBM) else pltpu.with_memory_space_constraint(a, HBM)
    result = lambda s, d, p, *at: at[0](s, d) if at else HBM(s, d) if p.memory_space == HBM else jax.ShapeDtypeStruct(s, d)
    return pl.pallas_call(
        body,
        grid=grid,
        in_specs=[i[1] for i in ins],
        out_specs=[o[2] for o in outs],
        out_shape=[result(*o) for o in outs],
        scratch_shapes=list(scratch),
        compiler_params=pltpu.CompilerParams(vmem_limit_bytes=LIMIT),
        cost_estimate=pl.CostEstimate(flops=flops, bytes_accessed=nbytes, transcendentals=0),
    )(*[place(*i) for i in ins])


def publish_body(boundary_hbm, nodes_hbm, out, boundary, nodes, sems):
    copies = [pltpu.make_async_copy(boundary_hbm, boundary, sems.at[0]), pltpu.make_async_copy(nodes_hbm, nodes, sems.at[1])]
    for copy in copies:
        copy.start()
    for copy in copies:
        copy.wait()
    hot = ones_where(iota((nodes.shape[0], boundary.shape[1]), 0) == boundary[...])
    out[...] = dot_t(hot, nodes[...]).astype(BF)


def before_body(sender, receiver, nodes, w_in, edges, ready, out, table_r, table_s):
    n, f = nodes.shape

    @pl.when(pl.program_id(0) == 0)
    def _():
        table_s[...] = dot(nodes[...], w_in[0:f, :]).astype(BF)
        table_r[...] = dot(nodes[...], w_in[f : 2 * f, :]).astype(BF)

    total = dot(edges[...], w_in[2 * f : 3 * f, :])
    total += dot(rows_hot(sender[0], n), table_s[...])
    total += dot(rows_hot(receiver[0], n), table_r[...])
    out[...] = total


def grid_before_body(receiver, nodes, w_in, edges, ready, out, table_r):
    n, f = nodes.shape

    @pl.when(pl.program_id(0) == 0)
    def _():
        table_r[...] = dot(nodes[...], w_in[f : 2 * f, :]).astype(BF)

    out[...] = dot(edges[...], w_in[2 * f : 3 * f, :]) + dot(rows_hot(receiver[0], n), table_r[...])


def pieces_of(chips, offered):
    pair = 2 * offered
    far = [(2, 0), (-2, 1)]
    for step in range(STEPS + 1):
        far += [(LEAD + step, 0), (SEED + step, 0), (step - SEED, 1)]
    far += [(-LEAD, 1)]
    for step in range(1, STEPS + 1):
        far += [(-LEAD - step, 1), (-SEED - step, 1), (SEED - step, 0)]
    table = {}
    for i, (offset, flip) in enumerate(far):
        table.setdefault(offset % chips, (i * pair, flip))
    return table


def relative(sender, n, pair, chips, z, c):
    far = sender - n
    region = far // pair
    sign = 2 * c - 1
    offset = (sign * (region // 2 - z) + 2 * chips) % chips
    half = jnp.where(region % 2 == c, 0, 1)
    return far >= 0, region, offset, half, far % pair


def is_near(offset, chips):
    return (offset <= 1) | (offset == chips - 1)


def main_body(chips, first, place, live, sender, sender_row, receiver_row, need, w_s, both, up, down, edges, before, bias, w_out,
              gain, ready, *refs):
    totals, table = refs[-2:]
    z, c = place[0], place[1]
    n, _ = totals.shape
    step = pl.program_id(0)
    rows = edges.shape[0]
    pair, regions = need.shape
    offered = both.shape[0] // 2

    @pl.when(step == 0)
    def _():
        totals[...] = refs[0][...] if first else jnp.zeros_like(totals)
        r = iota((6 * pair, regions), 0)
        near = r // (2 * pair)
        half = (r // pair) % 2
        moved = jnp.where(near == 2, -1, near)
        chip = (z + (2 * c - 1) * moved + chips) % chips
        region = 2 * chip + jnp.where(half == 1, 1 - c, c)
        wanted = lax.dot_general(ones_where(iota((6 * pair, regions), 1) == region), need[...].astype(F32).astype(BF),
                                 (((1,), (1,)), ((), ())), preferred_element_type=F32)
        lane = iota((6 * pair, pair), 1) == iota((6 * pair, pair), 0) % pair
        column = jnp.sum(jnp.where(lane, wanted, 0.0), axis=1, keepdims=True).astype(I32)
        chosen = []
        for j, (source, flip) in enumerate(((both, 0), (up, 0), (down, 1))):
            own_half = iota((2 * pair, 2 * offered), 0) // pair
            at = (1 - own_half if flip else own_half) * offered + column[j * 2 * pair : (j + 1) * 2 * pair, :]
            chosen.append(dot(ones_where(iota((2 * pair, 2 * offered), 1) == at), source[...]))
        table[...] = dot(jnp.concatenate(chosen, axis=0).astype(BF), w_s[...]).astype(BF)

    remote, _, offset, half, slot = relative(sender[0], n, pair, chips, z, c)
    near = jnp.where(offset == chips - 1, 2, offset)
    place_of = jnp.where(remote & is_near(offset, chips), near * 2 * pair + half * pair + slot, -1)
    pre = before[...] + dot(rows_hot(place_of, 6 * pair), table[...])
    update = finish(pre, bias[...], w_out[...], gain[...])
    message = (edges[...].astype(F32) + update).astype(BF)
    position = (first + step) * rows + iota((1, rows), 1)
    remote, _, offset, _, _ = relative(sender_row[0], n, pair, chips, z, c)
    later = remote & jnp.logical_not(is_near(offset, chips))
    target = jnp.where((position < live[0]) & jnp.logical_not(later), receiver_row[0], -1)
    totals[...] += dot(ones_where(iota((n, rows), 0) == target), message)


def ahead_of(sources, targets, sems):
    copies = [pltpu.make_async_copy(a.at[pl.ds(0, b.shape[0]), :], b, sems.at[i]) for i, (a, b) in enumerate(zip(sources, targets))]
    for copy in copies:
        copy.start()
    return copies


def gathered(at, sources, starts):
    out = None
    for source, start in zip(sources, starts):
        hot = ones_where(iota((at.shape[0], source.shape[0]), 1) + start == at)
        part = dot(hot, source[...])
        out = part if out is None else out + part
    return out


def compact_body(chips, offered, starts, place, live, sender, receiver, need, w_in, table_r, edges, *refs):
    k, m = len(starts), AHEAD_FAR
    sources, ahead = refs[:k], refs[k : k + m]
    outs, count, near = refs[k + m : k + m + 5], refs[k + m + 5], refs[k + m + 6 : k + 2 * m + 6]
    kept, sems, ahead_sems = refs[-7:-2], refs[-2], refs[-1]
    pre, rows, source_rows, at_out, target_out = kept
    fetches = ahead_of(ahead, near, ahead_sems)
    z, c = place[0], place[1]
    groups = sender.shape[0]
    n, f = table_r.shape
    pair, regions = need.shape
    where_at = pieces_of(chips, offered)
    send = sender[...]
    remote, _, offset, _, _ = relative(send, n, pair, chips, z, c)
    position = iota((groups, 128), 0) * 128 + iota((groups, 128), 1)
    late = remote & jnp.logical_not(is_near(offset, chips)) & (position < live[0])
    late_bits = ones_where(late)
    within = dot(late_bits, ones_where(iota((128, 128), 0) < iota((128, 128), 1)))
    above = jnp.sum(dot(ones_where(iota((groups, groups), 1) < iota((groups, groups), 0)), late_bits), axis=1, keepdims=True)
    rank = jnp.where(late, (within + above).astype(I32), -1)
    total = jnp.sum(jnp.where(late, 1, 0))
    blocks = (total + 127) // 128
    count[0] = blocks

    def one(block, carry):
        base = pl.multiple_of(block * 128, 128)
        lines = pl.ds(base, 128)
        hot, send_at, receive_at = [], jnp.zeros((128, 128), I32), jnp.zeros((128, 128), I32)
        for g in range(groups):
            match = iota((128, 128), 0) + base == rank[g : g + 1, :]
            hot.append(ones_where(match))
            send_at += jnp.where(match, send[g : g + 1, :] + 1, 0)
            receive_at += jnp.where(match, receiver[g : g + 1, :] + 1, 0)
        edge = dot(jnp.concatenate(hot, axis=1), edges[...]).astype(BF)
        from_ = jnp.sum(send_at, axis=1, keepdims=True) - 1
        to = jnp.sum(receive_at, axis=1, keepdims=True) - 1
        valid, region, offset, half, slot = relative(from_, n, pair, chips, z, c)
        wanted = lax.dot_general(ones_where(iota((128, regions), 1) == region), need[...].astype(F32).astype(BF),
                                 (((1,), (1,)), ((), ())), preferred_element_type=F32)
        chosen = jnp.sum(jnp.where(iota((128, pair), 1) == slot, wanted, 0.0), axis=1, keepdims=True).astype(I32)
        start, flip = jnp.zeros((128, 1), I32), jnp.zeros((128, 1), I32)
        for key, (row, turned) in where_at.items():
            start = jnp.where(offset == key, row, start)
            flip = jnp.where(offset == key, turned, flip)
        at = jnp.where(valid, start + jnp.where(flip == 1, 1 - half, half) * offered + chosen, -1)
        rows[...] = edge
        pre[...] = dot(edge, w_in[2 * f : 3 * f, :]) + dot(ones_where(iota((128, n), 1) == to), table_r[...])
        source_rows[...] = gathered(at, sources, starts).astype(BF)
        at_out[...] = jnp.broadcast_to(at, (128, 128))
        target_out[...] = jnp.broadcast_to(to, (128, 128))
        copies = [pltpu.make_async_copy(v, o.at[lines, :], sems.at[i]) for i, (v, o) in enumerate(zip(kept, outs))]
        for copy in copies:
            copy.start()
        for copy in copies:
            copy.wait()
        return carry

    lax.fori_loop(0, blocks, one, 0)
    for fetch in fetches:
        fetch.wait()


def far_body(starts, count, nodes, boundary, totals, bias, gain, node_bias, node_gain, w_s, w_out, node_in, node_out, *refs):
    k, m = len(starts), AHEAD_GRID
    sources, stored, ahead = refs[:k], refs[k : k + 5], refs[k + 5 : k + 5 + m]
    result, kept_result, published = refs[k + 5 + m : k + 8 + m]
    near, acc = refs[k + 8 + m : k + 8 + 2 * m], refs[k + 8 + 2 * m]
    kept, late_sems, ahead_sems = refs[-7:-2], refs[-2], refs[-1]
    pre, rows, source_rows, at, target = kept
    n, f = nodes.shape

    def fetch(block, begin):
        lines = pl.ds(pl.multiple_of(block * 128, 128), 128)
        for i, (v, o) in enumerate(zip(stored, kept)):
            copy = pltpu.make_async_copy(v.at[lines, :], o, late_sems.at[i])
            copy.start() if begin else copy.wait()

    @pl.when(count[0] > 0)
    def _():
        fetch(0, True)

    fetches = ahead_of(ahead, near, ahead_sems)
    acc[...] = totals[...]

    def one(block, carry):
        fetch(block, False)
        source = (source_rows[...].astype(F32) + gathered(at[...][:, 0:1], sources, starts)).astype(BF)
        update = finish(pre[...] + dot(source, w_s[...]), bias[...], w_out[...], gain[...])
        message = (rows[...].astype(F32) + update).astype(BF)
        eye = iota((128, 128), 0) == iota((128, 128), 1)
        to = jnp.sum(jnp.where(eye, target[...] + 1, 0), axis=0, keepdims=True) - 1
        acc[...] += dot(ones_where(iota((n, 128), 0) == to), message)

        @pl.when(block + 1 < count[0])
        def _():
            fetch(block + 1, True)

        return carry

    lax.fori_loop(0, count[0], one, 0)
    pre_node = dot(nodes[...], node_in[0:f, :]) + dot(acc[...].astype(BF), node_in[f : 2 * f, :])
    update = finish(pre_node, node_bias[...], node_out[...], node_gain[...])
    value = (nodes[...].astype(F32) + update).astype(BF)
    result[...] = value
    kept_result[...] = value
    hot = ones_where(iota((n, boundary.shape[1]), 0) == boundary[...])
    published[...] = dot_t(hot, value).astype(BF)
    for copy in fetches:
        copy.wait()


def grid_local_body(sender, mesh_out, w_s, before, out, table):
    n = mesh_out.shape[0]

    @pl.when(pl.program_id(0) == 0)
    def _():
        table[...] = dot(mesh_out[...], w_s[...]).astype(BF)

    out[...] = before[...] + dot(rows_hot(sender[0], n), table[...])


def grid_body(mesh_count, pair, sender, receiver_row, wanted, a, b, c, d, w_s, nodes, edges, before, bias, w_out, gain,
              node_in, node_bias, node_out, node_gain, result, totals, table):
    n, f = nodes.shape
    step = pl.program_id(0)
    rows = edges.shape[0]

    @pl.when(step == 0)
    def _():
        pieces = []
        for j, block in enumerate((a, b, c, d)):
            hot = ones_where(iota((block.shape[0], pair), 0) == wanted[j : j + 1, :])
            pieces.append(dot_t(hot, block[...]))
        chosen = jnp.concatenate(pieces, axis=0).astype(BF)
        table[...] = dot(chosen, w_s[...]).astype(BF)

    pre = before[...] + dot(rows_hot(sender[0] - mesh_count, table.shape[0]), table[...])
    update = finish(pre, bias[...], w_out[...], gain[...])
    message = (edges[...].astype(F32) + update).astype(BF)
    part = dot(ones_where(iota((n, rows), 0) == receiver_row[0]), message)

    @pl.when(step == 0)
    def _():
        totals[...] = part

    @pl.when(step > 0)
    def _():
        totals[...] += part

    @pl.when(step == pl.num_programs(0) - 1)
    def _():
        summed = totals[...].astype(BF)
        pre = dot(nodes[...], node_in[0:f, :]) + dot(summed, node_in[f : 2 * f, :])
        update = finish(pre, node_bias[...], node_out[...], node_gain[...])
        result[...] = (nodes[...].astype(F32) + update).astype(BF)


def local(
    mesh_nodes,
    mesh_edges,
    grid_nodes,
    grid_edges,
    boundary,
    mesh_need,
    mesh_sender,
    mesh_receiver,
    mesh_live,
    grid_need,
    grid_sender,
    grid_receiver,
    process_edge_in,
    process_edge_bias,
    process_edge_out,
    process_edge_gain,
    process_node_in,
    process_node_bias,
    process_node_out,
    process_node_gain,
    decode_edge_in,
    decode_edge_bias,
    decode_edge_out,
    decode_edge_gain,
    decode_node_in,
    decode_node_bias,
    decode_node_out,
    decode_node_gain,
):
    chips = lax.axis_size("z")
    regions = 2 * chips
    place = jnp.stack([lax.axis_index("z"), lax.axis_index("core")]).astype(I32)
    n, f = mesh_nodes.shape
    edges = mesh_edges.shape[0]
    grid_n = grid_nodes.shape[0]
    grid_e = grid_edges.shape[0]
    offered = boundary.shape[1]
    pair = mesh_need.shape[2]
    smem = pl.BlockSpec(memory_space=pltpu.SMEM)
    row = lambda v: v.reshape(1, -1)
    mesh_steps = edges // BLOCK
    grid_steps = grid_e // GRID_BLOCK
    as_blocks = lambda v, b: v.reshape(-1, b // 128, 128)
    as_rows = lambda v, b: v.reshape(-1, 1, b)
    idx_spec = lambda b: pl.BlockSpec((1, b // 128, 128), lambda i: (i, 0, 0))
    row_spec = lambda b: pl.BlockSpec((1, 1, b), lambda i: (i, 0, 0))
    tile = lambda b: pl.BlockSpec((b, f), lambda i: (i, 0))
    full = lambda v: (v, whole(v.shape))
    held = lambda v: (v, whole(v.shape), True)

    def along(steps):
        pairs = []
        for z in range(chips):
            pairs.append((2 * z, 2 * ((z + steps) % chips)))
            pairs.append((2 * z + 1, 2 * ((z - steps) % chips) + 1))
        return pairs

    def shift(v, steps):
        return lax.ppermute(v, REGION, along(steps))

    def swap(v):
        return lax.ppermute(v, "core", [(0, 1), (1, 0)])

    hbm = pl.BlockSpec(memory_space=HBM)
    anywhere = pl.BlockSpec(memory_space=pl.ANY)
    need = jnp.transpose(mesh_need[0])
    send_rows = mesh_sender.reshape(-1, 128)
    receive_rows = mesh_receiver.reshape(-1, 128)

    (own,) = call(publish_body, (1,), [(boundary, hbm), (mesh_nodes, hbm)], [((offered, f), BF, whole((offered, f)))],
                  [pltpu.VMEM((1, offered), I32), pltpu.VMEM((n, f), BF), pltpu.SemaphoreType.DMA((2,))],
                  flops=2 * offered * n * f, nbytes=2 * n * f)
    both = jnp.concatenate([own, swap(own)], axis=0)
    lead = [both]
    lead.append(shift(both, 1))
    seed = shift(both, SEED)
    lead.append(shift(lead[1], 1))
    lead.append(shift(lead[2], 1))
    back = [None]
    for k in range(1, LEAD + 1):
        back.append(swap(lead[k]))
    seed_back = swap(seed)
    before, table_r = call(
        before_body, (mesh_steps,),
        [(as_blocks(mesh_sender, BLOCK), idx_spec(BLOCK)), (as_blocks(mesh_receiver, BLOCK), idx_spec(BLOCK)), full(mesh_nodes),
         full(process_edge_in), (mesh_edges, tile(BLOCK)), (lead[1], anywhere)],
        [((edges, f), F32, tile(BLOCK), HBM), ((n, f), BF, whole((n, f)))],
        [pltpu.VMEM((n, f), BF)],
        flops=2 * f * f * (edges * 3 + 2 * n), nbytes=6 * edges * f,
    )
    halves = mesh_steps // 2
    ready = lead[2]
    current = jnp.concatenate([lead[3], seed, seed_back], axis=0)
    chain, turned = [current], []
    for _ in range(STEPS):
        chain.append(shift(chain[-1], 1))
        turned.append(swap(chain[-1]))
    for part in range(2):
        first = part * halves
        at = lambda spec_rows, rank: pl.BlockSpec((1,) + spec_rows, lambda i: (i + first,) + (0,) * rank)
        moved = pl.BlockSpec((BLOCK, f), lambda i: (i + first, 0))
        (totals,) = call(
            functools.partial(main_body, chips, first), (halves,),
            [(place, smem), (mesh_live, smem), (as_blocks(mesh_sender, BLOCK), at((BLOCK // 128, 128), 2)),
             (as_rows(mesh_sender, BLOCK), at((1, BLOCK), 2)), (as_rows(mesh_receiver, BLOCK), at((1, BLOCK), 2)), full(need),
             (process_edge_in, whole((f, f))), held(lead[0]), held(lead[1]), held(back[1]), (mesh_edges, moved),
             (before, moved), full(row(process_edge_bias)), full(process_edge_out), full(row(process_edge_gain)),
             (ready, anywhere)] + ([full(totals)] if part else []),
            [((n, f), F32, whole((n, f)), HBM)],
            [pltpu.VMEM((6 * pair, f), BF)],
            flops=2 * f * f * halves * BLOCK * 2, nbytes=6 * halves * BLOCK * f,
        )
        ready = chain[0]
    (grid_before,) = call(
        grid_before_body, (grid_steps,),
        [(as_rows(grid_receiver, GRID_BLOCK), row_spec(GRID_BLOCK)), full(grid_nodes), full(decode_edge_in),
         (grid_edges, tile(GRID_BLOCK)), (chain[1], anywhere)],
        [((grid_e, f), F32, tile(GRID_BLOCK), HBM)],
        [pltpu.VMEM((grid_n, f), BF)],
        flops=2 * f * f * (grid_e * 2 + grid_n), nbytes=6 * grid_e * f,
    )
    far = [lead[2], back[2]] + chain + [back[3]] + turned
    starts, at_row = [], 0
    for v in far:
        starts.append(at_row)
        at_row += v.shape[0]
    last = [STEPS + 2, len(far) - 2, len(far) - 1]
    early = [i for i in range(len(far)) if i not in last]
    late_buffers = [pltpu.VMEM((128, f), F32), pltpu.VMEM((128, f), BF), pltpu.VMEM((128, f), BF), pltpu.VMEM((128, 128), I32),
                    pltpu.VMEM((128, 128), I32)]
    vmem = lambda v: ((f if v is process_edge_in or v is decode_edge_in else v.shape[0], f), v.dtype, pl.BlockSpec(memory_space=VMEM), VMEM)
    far_needs = [mesh_nodes, totals, process_edge_in, process_edge_out, process_node_in, process_node_out]
    grid_needs = [grid_before, decode_edge_in, grid_nodes, grid_edges, decode_edge_out, decode_node_in, decode_node_out]
    *stored, count, nodes_near, totals_near, head_near, out_near, node_in_near, node_out_near = call(
        functools.partial(compact_body, chips, offered, tuple(starts[i] for i in early)), (1,),
        [(place, smem), (mesh_live, smem), full(send_rows), full(receive_rows), full(need), full(process_edge_in), held(table_r),
         full(mesh_edges)] + [held(far[i]) for i in early] + [(v, hbm) for v in far_needs],
        [((edges, f), F32, hbm), ((edges, f), BF, hbm), ((edges, f), BF, hbm), ((edges, 128), I32, hbm),
         ((edges, 128), I32, hbm), ((1,), I32, smem)] + [vmem(v) for v in far_needs],
        late_buffers + [pltpu.SemaphoreType.DMA((5,)), pltpu.SemaphoreType.DMA((AHEAD_FAR,))],
        flops=2 * f * 128 * (edges + 4 * f), nbytes=2 * edges * f,
    )
    mesh_out, mesh_kept, published, grid_before, grid_head, nodes_g, edges_g, out_g, node_in_g, node_out_g = call(
        functools.partial(far_body, tuple(starts[i] for i in last)), (1,),
        [(count, smem), held(nodes_near), full(boundary), held(totals_near), full(row(process_edge_bias)),
         full(row(process_edge_gain)), full(row(process_node_bias)), full(row(process_node_gain)), held(head_near), held(out_near),
         held(node_in_near), held(node_out_near)] + [held(far[i]) for i in last] + [(v, hbm) for v in stored]
        + [(v, hbm) for v in grid_needs],
        [((n, f), BF, whole((n, f))), ((n, f), BF, whole((n, f)), VMEM), ((offered, f), BF, whole((offered, f)), VMEM)]
        + [vmem(v) for v in grid_needs],
        [pltpu.VMEM((n, f), F32)] + late_buffers + [pltpu.SemaphoreType.DMA((5,)), pltpu.SemaphoreType.DMA((AHEAD_GRID,))],
        flops=2 * f * f * 4 * n, nbytes=8 * n * f,
    )
    pieces = []
    for offset in (-2, -1, 1, 2):
        pieces.append(lax.ppermute(published, REGION, [(s, (s - offset) % regions) for s in range(regions)]))
    (grid_local,) = call(
        grid_local_body, (grid_steps,),
        [(as_rows(grid_sender, GRID_BLOCK), row_spec(GRID_BLOCK)), held(mesh_kept), held(grid_head),
         (grid_before, tile(GRID_BLOCK), True)],
        [((grid_e, f), F32, tile(GRID_BLOCK), VMEM)],
        [pltpu.VMEM((n, f), BF)],
        flops=2 * f * f * (grid_e + n), nbytes=8 * grid_e * f,
    )
    (grid_out,) = call(
        functools.partial(grid_body, n, pair), (grid_steps,),
        [(as_rows(grid_sender, GRID_BLOCK), row_spec(GRID_BLOCK)), (as_rows(grid_receiver, GRID_BLOCK), row_spec(GRID_BLOCK)),
         full(grid_need[0]), held(pieces[0]), held(pieces[1]), held(pieces[2]), held(pieces[3]),
         held(grid_head), held(nodes_g), (edges_g, tile(GRID_BLOCK), True), (grid_local, tile(GRID_BLOCK), True),
         full(row(decode_edge_bias)), held(out_g), full(row(decode_edge_gain)), held(node_in_g),
         full(row(decode_node_bias)), held(node_out_g), full(row(decode_node_gain))],
        [((grid_n, f), BF, whole((grid_n, f)))],
        [pltpu.VMEM((grid_n, f), F32), pltpu.VMEM((4 * pair, f), BF)],
        flops=2 * f * f * (grid_e * 2 + 3 * grid_n), nbytes=6 * grid_e * f,
    )
    return (mesh_out, grid_out)


def solution(mesh):
    cores = 2
    finer = Mesh(
        mesh.devices.reshape(mesh.shape["member"], mesh.shape["region"] // cores, cores), ("member", "z", "core")
    )
    in_specs = (
        P(MEMBER_REGION, None),
        P(REGION, None),
        P(MEMBER_REGION, None),
        P(REGION, None),
        P(REGION, None),
        P(REGION, None, None),
        P(REGION, None),
        P(REGION, None),
        P(REGION),
        P(REGION, None, None),
        P(REGION, None),
        P(REGION, None),
    ) + (P(),) * 16
    out_specs = (P(MEMBER_REGION, None), P(MEMBER_REGION, None))

    return jax.shard_map(local, mesh=finer, in_specs=in_specs, out_specs=out_specs, check_vma=False)
```

```python
import functools

import jax
import jax.numpy as jnp
from jax import lax
from jax.experimental import pallas as pl
from jax.experimental.pallas import tpu as pltpu
from jax.sharding import Mesh
from jax.sharding import PartitionSpec as P

REGION = ("z", "core")
MEMBER_REGION = ("member", "z", "core")
BF = jnp.bfloat16
F32 = jnp.float32
I32 = jnp.int32
HBM = pltpu.MemorySpace.HBM
VMEM = pltpu.MemorySpace.VMEM
SEED = 12
LEAD = 3
STEPS = 4
LATE = 256
AHEAD_MESH = 4
AHEAD_FAR = 2
AHEAD_GRID = 7
BLOCK = 512
GRID_BLOCK = 384
LIMIT = 24 * 2**20


def iota(shape, dim):
    return lax.broadcasted_iota(I32, shape, dim)


def ones_where(mask):
    return jnp.where(mask, 1.0, 0.0).astype(BF)


def dot(a, b):
    return jnp.dot(a, b, preferred_element_type=F32)


def dot_t(a, b):
    return lax.dot_general(a, b, (((0,), (0,)), ((), ())), preferred_element_type=F32)


def columns(rows):
    lines = [rows[i : i + 1, j : j + 128] for i in range(rows.shape[0]) for j in range(0, rows.shape[1], 128)]
    eye = iota((128, 128), 0) == iota((128, 128), 1)
    return [jnp.sum(jnp.where(eye, jnp.broadcast_to(line, (128, 128)), 0), axis=1, keepdims=True) for line in lines]


def rows_hot(rows, count):
    return jnp.concatenate([ones_where(iota((128, count), 1) == c) for c in columns(rows)], axis=0)


def silu(x):
    return x * (0.5 + 0.5 * jnp.tanh(0.5 * x))


def finish(pre, bias, w_out, gain):
    hidden = silu(pre + bias).astype(BF)
    y = dot(hidden, w_out)
    y = y - jnp.mean(y, axis=1, keepdims=True)
    spread = jnp.mean(y * y, axis=1, keepdims=True)
    return y * lax.rsqrt(spread + 0.25) * gain


def whole(shape):
    return pl.BlockSpec(shape, lambda *_: (0,) * len(shape))


def call(body, grid, ins, outs, scratch=(), flops=0, nbytes=0):
    place = lambda a, s, *near: a if near or s.memory_space not in (None, HBM) else pltpu.with_memory_space_constraint(a, HBM)
    result = lambda s, d, p, *at: at[0](s, d) if at else HBM(s, d) if p.memory_space == HBM else jax.ShapeDtypeStruct(s, d)
    return pl.pallas_call(
        body,
        grid=grid,
        in_specs=[i[1] for i in ins],
        out_specs=[o[2] for o in outs],
        out_shape=[result(*o) for o in outs],
        scratch_shapes=list(scratch),
        compiler_params=pltpu.CompilerParams(vmem_limit_bytes=LIMIT),
        cost_estimate=pl.CostEstimate(flops=flops, bytes_accessed=nbytes, transcendentals=0),
    )(*[place(*i) for i in ins])


def publish_body(boundary_hbm, nodes_hbm, out, boundary, nodes, sems):
    copies = [pltpu.make_async_copy(boundary_hbm, boundary, sems.at[0]), pltpu.make_async_copy(nodes_hbm, nodes, sems.at[1])]
    for copy in copies:
        copy.start()
    for copy in copies:
        copy.wait()
    hot = ones_where(iota((nodes.shape[0], boundary.shape[1]), 0) == boundary[...])
    out[...] = dot_t(hot, nodes[...]).astype(BF)


def before_body(sender, receiver, nodes, w_in, edges, ready, out, table_r, table_s):
    n, f = nodes.shape

    @pl.when(pl.program_id(0) == 0)
    def _():
        table_s[...] = dot(nodes[...], w_in[0:f, :]).astype(BF)
        table_r[...] = dot(nodes[...], w_in[f : 2 * f, :]).astype(BF)

    total = dot(edges[...], w_in[2 * f : 3 * f, :])
    total += dot(rows_hot(sender[0], n), table_s[...])
    total += dot(rows_hot(receiver[0], n), table_r[...])
    out[...] = total


def grid_before_body(receiver, nodes, w_in, edges, ready, *refs):
    m = AHEAD_MESH
    ahead, out, near, table_r, sems = refs[:m], refs[m], refs[m + 1 : 2 * m + 1], refs[-2], refs[-1]
    n, f = nodes.shape

    @pl.when(pl.program_id(0) == 0)
    def _():
        ahead_of(ahead, near, sems)
        table_r[...] = dot(nodes[...], w_in[f : 2 * f, :]).astype(BF)

    out[...] = dot(edges[...], w_in[2 * f : 3 * f, :]) + dot(rows_hot(receiver[0], n), table_r[...])

    @pl.when(pl.program_id(0) == pl.num_programs(0) - 1)
    def _():
        for copy in ahead_of(ahead, near, sems, False):
            copy.wait()


def pieces_of(chips, offered):
    pair = 2 * offered
    far = [(2, 0), (-2, 1)]
    for step in range(STEPS + 1):
        far += [(LEAD + step, 0), (SEED + step, 0), (step - SEED, 1)]
    far += [(-LEAD, 1)]
    for step in range(1, STEPS + 1):
        far += [(-LEAD - step, 1), (-SEED - step, 1), (SEED - step, 0)]
    table = {}
    for i, (offset, flip) in enumerate(far):
        table.setdefault(offset % chips, (i * pair, flip))
    return table


def relative(sender, n, pair, chips, z, c):
    far = sender - n
    region = far // pair
    sign = 2 * c - 1
    offset = (sign * (region // 2 - z) + 2 * chips) % chips
    half = jnp.where(region % 2 == c, 0, 1)
    return far >= 0, region, offset, half, far % pair


def is_near(offset, chips):
    return (offset <= 1) | (offset == chips - 1)


def main_body(chips, first, place, live, sender, sender_row, receiver_row, need, w_s, both, up, down, edges, before, bias, w_out,
              gain, ready, *refs):
    totals, table = refs[-2:]
    z, c = place[0], place[1]
    n, _ = totals.shape
    step = pl.program_id(0)
    rows = edges.shape[0]
    pair, regions = need.shape
    offered = both.shape[0] // 2

    @pl.when(step == 0)
    def _():
        totals[...] = refs[0][...] if first else jnp.zeros_like(totals)
        r = iota((6 * pair, regions), 0)
        near = r // (2 * pair)
        half = (r // pair) % 2
        moved = jnp.where(near == 2, -1, near)
        chip = (z + (2 * c - 1) * moved + chips) % chips
        region = 2 * chip + jnp.where(half == 1, 1 - c, c)
        wanted = lax.dot_general(ones_where(iota((6 * pair, regions), 1) == region), need[...].astype(F32).astype(BF),
                                 (((1,), (1,)), ((), ())), preferred_element_type=F32)
        lane = iota((6 * pair, pair), 1) == iota((6 * pair, pair), 0) % pair
        column = jnp.sum(jnp.where(lane, wanted, 0.0), axis=1, keepdims=True).astype(I32)
        chosen = []
        for j, (source, flip) in enumerate(((both, 0), (up, 0), (down, 1))):
            own_half = iota((2 * pair, 2 * offered), 0) // pair
            at = (1 - own_half if flip else own_half) * offered + column[j * 2 * pair : (j + 1) * 2 * pair, :]
            chosen.append(dot(ones_where(iota((2 * pair, 2 * offered), 1) == at), source[...]))
        table[...] = dot(jnp.concatenate(chosen, axis=0).astype(BF), w_s[...]).astype(BF)

    remote, _, offset, half, slot = relative(sender[0], n, pair, chips, z, c)
    near = jnp.where(offset == chips - 1, 2, offset)
    place_of = jnp.where(remote & is_near(offset, chips), near * 2 * pair + half * pair + slot, -1)
    pre = before[...] + dot(rows_hot(place_of, 6 * pair), table[...])
    update = finish(pre, bias[...], w_out[...], gain[...])
    message = (edges[...].astype(F32) + update).astype(BF)
    position = (first + step) * rows + iota((1, rows), 1)
    remote, _, offset, _, _ = relative(sender_row[0], n, pair, chips, z, c)
    later = remote & jnp.logical_not(is_near(offset, chips))
    target = jnp.where((position < live[0]) & jnp.logical_not(later), receiver_row[0], -1)
    totals[...] += dot(ones_where(iota((n, rows), 0) == target), message)


def ahead_of(sources, targets, sems, begin=True):
    copies = [pltpu.make_async_copy(a.at[pl.ds(0, b.shape[0]), :], b, sems.at[i]) for i, (a, b) in enumerate(zip(sources, targets))]
    for copy in copies if begin else ():
        copy.start()
    return copies


def gathered(at, sources, starts):
    out = None
    for source, start in zip(sources, starts):
        hot = ones_where(iota((at.shape[0], source.shape[0]), 1) + start == at)
        part = dot(hot, source[...])
        out = part if out is None else out + part
    return out


def compact_body(chips, offered, starts, place, live, sender, receiver, need, w_e, table_r, edges, *refs):
    k, m = len(starts), AHEAD_FAR
    sources, ahead = refs[:k], refs[k : k + m]
    outs, count, near = refs[k + m : k + m + 5], refs[k + m + 5], refs[k + m + 6 : k + 2 * m + 6]
    ahead_sems = refs[-1]
    pre, rows, source_rows, at_out, target_out = outs
    fetches = ahead_of(ahead, near, ahead_sems)
    z, c = place[0], place[1]
    groups = sender.shape[0]
    n, _ = table_r.shape
    pair, regions = need.shape
    where_at = pieces_of(chips, offered)
    send = sender[...]
    remote, _, offset, _, _ = relative(send, n, pair, chips, z, c)
    position = iota((groups, 128), 0) * 128 + iota((groups, 128), 1)
    late = remote & jnp.logical_not(is_near(offset, chips)) & (position < live[0])
    late_bits = ones_where(late)
    within = dot(late_bits, ones_where(iota((128, 128), 0) < iota((128, 128), 1)))
    above = jnp.sum(dot(ones_where(iota((groups, groups), 1) < iota((groups, groups), 0)), late_bits), axis=1, keepdims=True)
    rank = jnp.where(late, (within + above).astype(I32), -1)
    total = jnp.sum(jnp.where(late, 1, 0))
    blocks = (total + LATE - 1) // LATE
    count[0] = blocks

    def one(block, carry):
        base = pl.multiple_of(block * LATE, LATE)
        lines = pl.ds(base, LATE)
        hot, send_at, receive_at = [], jnp.zeros((LATE, 128), I32), jnp.zeros((LATE, 128), I32)
        for g in range(groups):
            match = iota((LATE, 128), 0) + base == rank[g : g + 1, :]
            hot.append(ones_where(match))
            send_at += jnp.where(match, send[g : g + 1, :] + 1, 0)
            receive_at += jnp.where(match, receiver[g : g + 1, :] + 1, 0)
        edge = dot(jnp.concatenate(hot, axis=1), edges[...]).astype(BF)
        from_ = jnp.sum(send_at, axis=1, keepdims=True) - 1
        to = jnp.sum(receive_at, axis=1, keepdims=True) - 1
        valid, region, offset, half, slot = relative(from_, n, pair, chips, z, c)
        wanted = lax.dot_general(ones_where(iota((LATE, regions), 1) == region), need[...].astype(F32).astype(BF),
                                 (((1,), (1,)), ((), ())), preferred_element_type=F32)
        chosen = jnp.sum(jnp.where(iota((LATE, pair), 1) == slot, wanted, 0.0), axis=1, keepdims=True).astype(I32)
        start, flip = jnp.zeros((LATE, 1), I32), jnp.zeros((LATE, 1), I32)
        for key, (row, turned) in where_at.items():
            start = jnp.where(offset == key, row, start)
            flip = jnp.where(offset == key, turned, flip)
        at = jnp.where(valid, start + jnp.where(flip == 1, 1 - half, half) * offered + chosen, -1)
        rows[lines, :] = edge
        pre[lines, :] = dot(edge, w_e[...]) + dot(ones_where(iota((LATE, n), 1) == to), table_r[...])
        source_rows[lines, :] = gathered(at, sources, starts).astype(BF)
        at_out[lines, :] = jnp.broadcast_to(at, (LATE, 128))
        target_out[lines, :] = jnp.broadcast_to(to, (LATE, 128))
        return carry

    lax.fori_loop(0, blocks, one, 0)
    for fetch in fetches:
        fetch.wait()


def far_body(starts, count, nodes, boundary, totals, bias, gain, node_bias, node_gain, w_s, w_out, node_in, node_out, *refs):
    k, m = len(starts), AHEAD_GRID
    sources, (pre, rows, source_rows, at, target), ahead = refs[:k], refs[k : k + 5], refs[k + 5 : k + 5 + m]
    result, kept_result, published = refs[k + 5 + m : k + 8 + m]
    near, acc, ahead_sems = refs[k + 8 + m : k + 8 + 2 * m], refs[-2], refs[-1]
    n, f = nodes.shape
    fetches = ahead_of(ahead, near, ahead_sems)
    acc[...] = totals[...]

    def one(block, carry):
        lines = pl.ds(pl.multiple_of(block * LATE, LATE), LATE)
        source = (source_rows[lines, :].astype(F32) + gathered(at[lines, :][:, 0:1], sources, starts)).astype(BF)
        update = finish(pre[lines, :] + dot(source, w_s[...]), bias[...], w_out[...], gain[...])
        message = (rows[lines, :].astype(F32) + update).astype(BF)
        eye = iota((128, 128), 0) == iota((128, 128), 1)
        targets = target[lines, :] + 1
        to = [jnp.sum(jnp.where(eye, targets[i : i + 128, :], 0), axis=0, keepdims=True) for i in range(0, LATE, 128)]
        acc[...] += dot(ones_where(iota((n, LATE), 0) + 1 == jnp.concatenate(to, axis=1)), message)
        return carry

    lax.fori_loop(0, count[0], one, 0)
    pre_node = dot(nodes[...], node_in[0:f, :]) + dot(acc[...].astype(BF), node_in[f : 2 * f, :])
    update = finish(pre_node, node_bias[...], node_out[...], node_gain[...])
    value = (nodes[...].astype(F32) + update).astype(BF)
    result[...] = value
    kept_result[...] = value
    hot = ones_where(iota((n, boundary.shape[1]), 0) == boundary[...])
    published[...] = dot_t(hot, value).astype(BF)
    for copy in fetches:
        copy.wait()


def grid_local_body(sender, mesh_out, w_s, before, out, table):
    n = mesh_out.shape[0]

    @pl.when(pl.program_id(0) == 0)
    def _():
        table[...] = dot(mesh_out[...], w_s[...]).astype(BF)

    out[...] = before[...] + dot(rows_hot(sender[0], n), table[...])


def grid_body(mesh_count, pair, sender, receiver_row, wanted, a, b, c, d, w_s, nodes, edges, before, bias, w_out, gain,
              node_in, node_bias, node_out, node_gain, result, totals, table):
    n, f = nodes.shape
    step = pl.program_id(0)
    rows = edges.shape[0]

    @pl.when(step == 0)
    def _():
        pieces = []
        for j, block in enumerate((a, b, c, d)):
            hot = ones_where(iota((block.shape[0], pair), 0) == wanted[j : j + 1, :])
            pieces.append(dot_t(hot, block[...]))
        chosen = jnp.concatenate(pieces, axis=0).astype(BF)
        table[...] = dot(chosen, w_s[...]).astype(BF)

    pre = before[...] + dot(rows_hot(sender[0] - mesh_count, table.shape[0]), table[...])
    update = finish(pre, bias[...], w_out[...], gain[...])
    message = (edges[...].astype(F32) + update).astype(BF)
    part = dot(ones_where(iota((n, rows), 0) == receiver_row[0]), message)

    @pl.when(step == 0)
    def _():
        totals[...] = part

    @pl.when(step > 0)
    def _():
        totals[...] += part

    @pl.when(step == pl.num_programs(0) - 1)
    def _():
        summed = totals[...].astype(BF)
        pre = dot(nodes[...], node_in[0:f, :]) + dot(summed, node_in[f : 2 * f, :])
        update = finish(pre, node_bias[...], node_out[...], node_gain[...])
        result[...] = (nodes[...].astype(F32) + update).astype(BF)


def local(
    mesh_nodes,
    mesh_edges,
    grid_nodes,
    grid_edges,
    boundary,
    mesh_need,
    mesh_sender,
    mesh_receiver,
    mesh_live,
    grid_need,
    grid_sender,
    grid_receiver,
    process_edge_in,
    process_edge_bias,
    process_edge_out,
    process_edge_gain,
    process_node_in,
    process_node_bias,
    process_node_out,
    process_node_gain,
    decode_edge_in,
    decode_edge_bias,
    decode_edge_out,
    decode_edge_gain,
    decode_node_in,
    decode_node_bias,
    decode_node_out,
    decode_node_gain,
):
    chips = lax.axis_size("z")
    regions = 2 * chips
    place = jnp.stack([lax.axis_index("z"), lax.axis_index("core")]).astype(I32)
    n, f = mesh_nodes.shape
    edges = mesh_edges.shape[0]
    grid_n = grid_nodes.shape[0]
    grid_e = grid_edges.shape[0]
    offered = boundary.shape[1]
    pair = mesh_need.shape[2]
    smem = pl.BlockSpec(memory_space=pltpu.SMEM)
    row = lambda v: v.reshape(1, -1)
    mesh_steps = edges // BLOCK
    grid_steps = grid_e // GRID_BLOCK
    as_blocks = lambda v, b: v.reshape(-1, b // 128, 128)
    as_rows = lambda v, b: v.reshape(-1, 1, b)
    idx_spec = lambda b: pl.BlockSpec((1, b // 128, 128), lambda i: (i, 0, 0))
    row_spec = lambda b: pl.BlockSpec((1, 1, b), lambda i: (i, 0, 0))
    tile = lambda b: pl.BlockSpec((b, f), lambda i: (i, 0))
    full = lambda v: (v, whole(v.shape))
    held = lambda v: (v, whole(v.shape), True)

    def along(steps):
        pairs = []
        for z in range(chips):
            pairs.append((2 * z, 2 * ((z + steps) % chips)))
            pairs.append((2 * z + 1, 2 * ((z - steps) % chips) + 1))
        return pairs

    def shift(v, steps):
        return lax.ppermute(v, REGION, along(steps))

    def swap(v):
        return lax.ppermute(v, "core", [(0, 1), (1, 0)])

    hbm = pl.BlockSpec(memory_space=HBM)
    anywhere = pl.BlockSpec(memory_space=pl.ANY)
    need = jnp.transpose(mesh_need[0])
    send_rows = mesh_sender.reshape(-1, 128)
    receive_rows = mesh_receiver.reshape(-1, 128)

    (own,) = call(publish_body, (1,), [(boundary, hbm), (mesh_nodes, hbm)], [((offered, f), BF, whole((offered, f)))],
                  [pltpu.VMEM((1, offered), I32), pltpu.VMEM((n, f), BF), pltpu.SemaphoreType.DMA((2,))],
                  flops=2 * offered * n * f, nbytes=2 * n * f)
    both = jnp.concatenate([own, swap(own)], axis=0)
    lead = [both]
    lead.append(shift(both, 1))
    seed = shift(both, SEED)
    lead.append(shift(lead[1], 1))
    lead.append(shift(lead[2], 1))
    back = [None]
    for k in range(1, LEAD + 1):
        back.append(swap(lead[k]))
    seed_back = swap(seed)
    vmem = lambda v: ((f if v is decode_edge_in else v.shape[0], f), v.dtype, pl.BlockSpec(memory_space=VMEM), VMEM)
    mesh_needs = [process_edge_in, mesh_nodes, mesh_edges, process_edge_out]
    grid_before, w_in_near, nodes_near, edges_near, out_near = call(
        grid_before_body, (grid_steps,),
        [(as_rows(grid_receiver, GRID_BLOCK), row_spec(GRID_BLOCK)), full(grid_nodes), full(decode_edge_in),
         (grid_edges, tile(GRID_BLOCK)), (lead[1], anywhere)] + [(v, hbm) for v in mesh_needs],
        [((grid_e, f), F32, tile(GRID_BLOCK), HBM)] + [vmem(v) for v in mesh_needs],
        [pltpu.VMEM((grid_n, f), BF), pltpu.SemaphoreType.DMA((AHEAD_MESH,))],
        flops=2 * f * f * (grid_e * 2 + grid_n), nbytes=6 * grid_e * f,
    )
    before, table_r = call(
        before_body, (mesh_steps,),
        [(as_blocks(mesh_sender, BLOCK), idx_spec(BLOCK)), (as_blocks(mesh_receiver, BLOCK), idx_spec(BLOCK)), held(nodes_near),
         held(w_in_near), (edges_near, tile(BLOCK), True), (lead[2], anywhere)],
        [((edges, f), F32, tile(BLOCK), VMEM), ((n, f), BF, whole((n, f)), VMEM)],
        [pltpu.VMEM((n, f), BF)],
        flops=2 * f * f * (edges * 3 + 2 * n), nbytes=6 * edges * f,
    )
    halves = mesh_steps // 2
    ready = lead[3]
    current = jnp.concatenate([lead[3], seed, seed_back], axis=0)
    chain, turned = [current], []
    for _ in range(STEPS):
        chain.append(shift(chain[-1], 1))
        turned.append(swap(chain[-1]))
    for part in range(2):
        first = part * halves
        at = lambda spec_rows, rank: pl.BlockSpec((1,) + spec_rows, lambda i: (i + first,) + (0,) * rank)
        moved = pl.BlockSpec((BLOCK, f), lambda i: (i + first, 0))
        (totals,) = call(
            functools.partial(main_body, chips, first), (halves,),
            [(place, smem), (mesh_live, smem), (as_blocks(mesh_sender, BLOCK), at((BLOCK // 128, 128), 2)),
             (as_rows(mesh_sender, BLOCK), at((1, BLOCK), 2)), (as_rows(mesh_receiver, BLOCK), at((1, BLOCK), 2)), full(need),
             (w_in_near, whole((f, f)), True), held(lead[0]), held(lead[1]), held(back[1]), (edges_near, moved, True),
             (before, moved, True), full(row(process_edge_bias)), held(out_near), full(row(process_edge_gain)),
             (ready, anywhere)] + ([held(totals)] if part else []),
            [((n, f), F32, whole((n, f)), VMEM)],
            [pltpu.VMEM((6 * pair, f), BF)],
            flops=2 * f * f * halves * BLOCK * 2, nbytes=6 * halves * BLOCK * f,
        )
        ready = chain[1]
    far = [lead[2], back[2]] + chain + [back[3]] + turned
    starts, at_row = [], 0
    for v in far:
        starts.append(at_row)
        at_row += v.shape[0]
    last = [STEPS + 2, len(far) - 2, len(far) - 1]
    early = [i for i in range(len(far)) if i not in last]
    far_needs = [process_node_in, process_node_out]
    grid_needs = [grid_before, decode_edge_in, grid_nodes, grid_edges, decode_edge_out, decode_node_in, decode_node_out]
    on_chip = lambda dtype, width: ((edges, width), dtype, pl.BlockSpec(memory_space=VMEM), VMEM)
    *stored, count, node_in_near, node_out_near = call(
        functools.partial(compact_body, chips, offered, tuple(starts[i] for i in early)), (1,),
        [(place, smem), (mesh_live, smem), full(send_rows), full(receive_rows), full(need),
         (w_in_near, pl.BlockSpec((f, f), lambda i: (2, 0)), True), held(table_r), held(edges_near)]
        + [held(far[i]) for i in early] + [(v, hbm) for v in far_needs],
        [on_chip(F32, f), on_chip(BF, f), on_chip(BF, f), on_chip(I32, 128), on_chip(I32, 128), ((1,), I32, smem)]
        + [vmem(v) for v in far_needs],
        [pltpu.SemaphoreType.DMA((AHEAD_FAR,))],
        flops=2 * f * 128 * (edges + 4 * f), nbytes=2 * edges * f,
    )
    mesh_out, mesh_kept, published, grid_before, grid_head, nodes_g, edges_g, out_g, node_in_g, node_out_g = call(
        functools.partial(far_body, tuple(starts[i] for i in last)), (1,),
        [(count, smem), held(nodes_near), full(boundary), held(totals), full(row(process_edge_bias)),
         full(row(process_edge_gain)), full(row(process_node_bias)), full(row(process_node_gain)), (w_in_near, whole((f, f)), True),
         held(out_near), held(node_in_near), held(node_out_near)] + [held(far[i]) for i in last]
        + [(v, pl.BlockSpec(memory_space=VMEM), True) for v in stored] + [(v, hbm) for v in grid_needs],
        [((n, f), BF, whole((n, f))), ((n, f), BF, whole((n, f)), VMEM), ((offered, f), BF, whole((offered, f)), VMEM)]
        + [vmem(v) for v in grid_needs],
        [pltpu.VMEM((n, f), F32), pltpu.SemaphoreType.DMA((AHEAD_GRID,))],
        flops=2 * f * f * 4 * n, nbytes=8 * n * f,
    )
    pieces = []
    for offset in (-2, -1, 1, 2):
        pieces.append(lax.ppermute(published, REGION, [(s, (s - offset) % regions) for s in range(regions)]))
    (grid_local,) = call(
        grid_local_body, (grid_steps,),
        [(as_rows(grid_sender, GRID_BLOCK), row_spec(GRID_BLOCK)), held(mesh_kept), held(grid_head),
         (grid_before, tile(GRID_BLOCK), True)],
        [((grid_e, f), F32, tile(GRID_BLOCK), VMEM)],
        [pltpu.VMEM((n, f), BF)],
        flops=2 * f * f * (grid_e + n), nbytes=8 * grid_e * f,
    )
    (grid_out,) = call(
        functools.partial(grid_body, n, pair), (grid_steps,),
        [(as_rows(grid_sender, GRID_BLOCK), row_spec(GRID_BLOCK)), (as_rows(grid_receiver, GRID_BLOCK), row_spec(GRID_BLOCK)),
         full(grid_need[0]), held(pieces[0]), held(pieces[1]), held(pieces[2]), held(pieces[3]),
         held(grid_head), held(nodes_g), (edges_g, tile(GRID_BLOCK), True), (grid_local, tile(GRID_BLOCK), True),
         full(row(decode_edge_bias)), held(out_g), full(row(decode_edge_gain)), held(node_in_g),
         full(row(decode_node_bias)), held(node_out_g), full(row(decode_node_gain))],
        [((grid_n, f), BF, whole((grid_n, f)))],
        [pltpu.VMEM((grid_n, f), F32), pltpu.VMEM((4 * pair, f), BF)],
        flops=2 * f * f * (grid_e * 2 + 3 * grid_n), nbytes=6 * grid_e * f,
    )
    return (mesh_out, grid_out)


def solution(mesh):
    cores = 2
    finer = Mesh(
        mesh.devices.reshape(mesh.shape["member"], mesh.shape["region"] // cores, cores), ("member", "z", "core")
    )
    in_specs = (
        P(MEMBER_REGION, None),
        P(REGION, None),
        P(MEMBER_REGION, None),
        P(REGION, None),
        P(REGION, None),
        P(REGION, None, None),
        P(REGION, None),
        P(REGION, None),
        P(REGION),
        P(REGION, None, None),
        P(REGION, None),
        P(REGION, None),
    ) + (P(),) * 16
    out_specs = (P(MEMBER_REGION, None), P(MEMBER_REGION, None))

    return jax.shard_map(local, mesh=finer, in_specs=in_specs, out_specs=out_specs, check_vma=False)
```

```python
import functools

import jax
import jax.numpy as jnp
from jax import lax
from jax.experimental import pallas as pl
from jax.experimental.pallas import tpu as pltpu
from jax.sharding import Mesh
from jax.sharding import PartitionSpec as P

REGION = ("z", "core")
MEMBER_REGION = ("member", "z", "core")
BF = jnp.bfloat16
F32 = jnp.float32
I32 = jnp.int32
HBM = pltpu.MemorySpace.HBM
VMEM = pltpu.MemorySpace.VMEM
SEED = 12
REACH = 7
STEPS = 4
LATE = 256
AHEAD_MESH = 4
AHEAD_FAR = 2
AHEAD_GRID = 7
BLOCK = 512
GRID_BLOCK = 384
LIMIT = 24 * 2**20


def iota(shape, dim):
    return lax.broadcasted_iota(I32, shape, dim)


def ones_where(mask):
    return jnp.where(mask, 1.0, 0.0).astype(BF)


def dot(a, b):
    return jnp.dot(a, b, preferred_element_type=F32)


def dot_t(a, b):
    return lax.dot_general(a, b, (((0,), (0,)), ((), ())), preferred_element_type=F32)


def columns(rows):
    lines = [rows[i : i + 1, j : j + 128] for i in range(rows.shape[0]) for j in range(0, rows.shape[1], 128)]
    eye = iota((128, 128), 0) == iota((128, 128), 1)
    return [jnp.sum(jnp.where(eye, jnp.broadcast_to(line, (128, 128)), 0), axis=1, keepdims=True) for line in lines]


def rows_hot(rows, count):
    return jnp.concatenate([ones_where(iota((128, count), 1) == c) for c in columns(rows)], axis=0)


def silu(x):
    return x * (0.5 + 0.5 * jnp.tanh(0.5 * x))


def finish(pre, bias, w_out, gain):
    hidden = silu(pre + bias).astype(BF)
    y = dot(hidden, w_out)
    y = y - jnp.mean(y, axis=1, keepdims=True)
    spread = jnp.mean(y * y, axis=1, keepdims=True)
    return y * lax.rsqrt(spread + 0.25) * gain


def whole(shape):
    return pl.BlockSpec(shape, lambda *_: (0,) * len(shape))


def call(body, grid, ins, outs, scratch=(), flops=0, nbytes=0):
    place = lambda a, s, *near: a if near or s.memory_space not in (None, HBM) else pltpu.with_memory_space_constraint(a, HBM)
    result = lambda s, d, p, *at: at[0](s, d) if at else HBM(s, d) if p.memory_space == HBM else jax.ShapeDtypeStruct(s, d)
    return pl.pallas_call(
        body,
        grid=grid,
        in_specs=[i[1] for i in ins],
        out_specs=[o[2] for o in outs],
        out_shape=[result(*o) for o in outs],
        scratch_shapes=list(scratch),
        compiler_params=pltpu.CompilerParams(vmem_limit_bytes=LIMIT),
        cost_estimate=pl.CostEstimate(flops=flops, bytes_accessed=nbytes, transcendentals=0),
    )(*[place(*i) for i in ins])


def publish_body(boundary_hbm, nodes_hbm, out, boundary, nodes, sems):
    copies = [pltpu.make_async_copy(boundary_hbm, boundary, sems.at[0]), pltpu.make_async_copy(nodes_hbm, nodes, sems.at[1])]
    for copy in copies:
        copy.start()
    for copy in copies:
        copy.wait()
    hot = ones_where(iota((nodes.shape[0], boundary.shape[1]), 0) == boundary[...])
    out[...] = dot_t(hot, nodes[...]).astype(BF)


def before_body(sender, receiver, nodes, w_in, edges, ready, out, table_r, table_s):
    n, f = nodes.shape

    @pl.when(pl.program_id(0) == 0)
    def _():
        table_s[...] = dot(nodes[...], w_in[0:f, :]).astype(BF)
        table_r[...] = dot(nodes[...], w_in[f : 2 * f, :]).astype(BF)

    total = dot(edges[...], w_in[2 * f : 3 * f, :])
    total += dot(rows_hot(sender[0], n), table_s[...])
    total += dot(rows_hot(receiver[0], n), table_r[...])
    out[...] = total


def grid_before_body(receiver, nodes, w_in, edges, ready, *refs):
    m = AHEAD_MESH
    ahead, out, near, table_r, sems = refs[:m], refs[m], refs[m + 1 : 2 * m + 1], refs[-2], refs[-1]
    n, f = nodes.shape

    @pl.when(pl.program_id(0) == 0)
    def _():
        ahead_of(ahead, near, sems)
        table_r[...] = dot(nodes[...], w_in[f : 2 * f, :]).astype(BF)

    out[...] = dot(edges[...], w_in[2 * f : 3 * f, :]) + dot(rows_hot(receiver[0], n), table_r[...])

    @pl.when(pl.program_id(0) == pl.num_programs(0) - 1)
    def _():
        for copy in ahead_of(ahead, near, sems, False):
            copy.wait()


def layout():
    lead = {("lead", k): [(k, 0)] for k in range(2, REACH + 1)}
    back = {("back", k): [(-k, 1)] for k in range(2, REACH + 1)}
    chain = {("chain", k): [(SEED + k, 0), (k - SEED, 1)] for k in range(STEPS + 1)}
    turn = {("turn", k): [(-SEED - k - 1, 1), (SEED - k - 1, 0)] for k in range(STEPS)}
    pieces = {**lead, **back, **chain, **turn}
    last = [("lead", REACH), ("back", REACH - 1), ("back", REACH), ("chain", STEPS), ("turn", STEPS - 2), ("turn", STEPS - 1)]
    return [(name, pieces[name]) for name in pieces if name not in last], [(name, pieces[name]) for name in last]


def pieces_of(chips, offered):
    early, last = layout()
    held = [item for _, items in early + last for item in items]
    table = {}
    for i, (offset, flip) in enumerate(held):
        table.setdefault(offset % chips, (i * 2 * offered, flip))
    return table


def relative(sender, n, pair, chips, z, c):
    far = sender - n
    region = far // pair
    sign = 2 * c - 1
    offset = (sign * (region // 2 - z) + 2 * chips) % chips
    half = jnp.where(region % 2 == c, 0, 1)
    return far >= 0, region, offset, half, far % pair


def is_near(offset, chips):
    return (offset <= 1) | (offset == chips - 1)


def main_body(chips, first, place, live, sender, sender_row, receiver_row, need, w_s, both, up, down, edges, before, bias, w_out,
              gain, ready, *refs):
    totals, table = refs[-2:]
    z, c = place[0], place[1]
    n, _ = totals.shape
    step = pl.program_id(0)
    rows = edges.shape[0]
    pair, regions = need.shape
    offered = both.shape[0] // 2

    @pl.when(step == 0)
    def _():
        totals[...] = refs[0][...] if first else jnp.zeros_like(totals)
        r = iota((6 * pair, regions), 0)
        near = r // (2 * pair)
        half = (r // pair) % 2
        moved = jnp.where(near == 2, -1, near)
        chip = (z + (2 * c - 1) * moved + chips) % chips
        region = 2 * chip + jnp.where(half == 1, 1 - c, c)
        wanted = lax.dot_general(ones_where(iota((6 * pair, regions), 1) == region), need[...].astype(F32).astype(BF),
                                 (((1,), (1,)), ((), ())), preferred_element_type=F32)
        lane = iota((6 * pair, pair), 1) == iota((6 * pair, pair), 0) % pair
        column = jnp.sum(jnp.where(lane, wanted, 0.0), axis=1, keepdims=True).astype(I32)
        chosen = []
        for j, (source, flip) in enumerate(((both, 0), (up, 0), (down, 1))):
            own_half = iota((2 * pair, 2 * offered), 0) // pair
            at = (1 - own_half if flip else own_half) * offered + column[j * 2 * pair : (j + 1) * 2 * pair, :]
            chosen.append(dot(ones_where(iota((2 * pair, 2 * offered), 1) == at), source[...]))
        table[...] = dot(jnp.concatenate(chosen, axis=0).astype(BF), w_s[...]).astype(BF)

    remote, _, offset, half, slot = relative(sender[0], n, pair, chips, z, c)
    near = jnp.where(offset == chips - 1, 2, offset)
    place_of = jnp.where(remote & is_near(offset, chips), near * 2 * pair + half * pair + slot, -1)
    pre = before[...] + dot(rows_hot(place_of, 6 * pair), table[...])
    update = finish(pre, bias[...], w_out[...], gain[...])
    message = (edges[...].astype(F32) + update).astype(BF)
    position = (first + step) * rows + iota((1, rows), 1)
    remote, _, offset, _, _ = relative(sender_row[0], n, pair, chips, z, c)
    later = remote & jnp.logical_not(is_near(offset, chips))
    target = jnp.where((position < live[0]) & jnp.logical_not(later), receiver_row[0], -1)
    totals[...] += dot(ones_where(iota((n, rows), 0) == target), message)


def ahead_of(sources, targets, sems, begin=True):
    copies = [pltpu.make_async_copy(a.at[pl.ds(0, b.shape[0]), :], b, sems.at[i]) for i, (a, b) in enumerate(zip(sources, targets))]
    for copy in copies if begin else ():
        copy.start()
    return copies


def gathered(at, sources, start):
    rows = jnp.concatenate([source[...] for source in sources], axis=0)
    return dot(ones_where(iota((at.shape[0], rows.shape[0]), 1) + start == at), rows)


def compact_body(chips, offered, k, place, live, sender, receiver, need, w_e, table_r, edges, *refs):
    m = AHEAD_FAR
    sources, ahead = refs[:k], refs[k : k + m]
    outs, count, near = refs[k + m : k + m + 5], refs[k + m + 5], refs[k + m + 6 : k + 2 * m + 6]
    ahead_sems = refs[-1]
    pre, rows, source_rows, at_out, target_out = outs
    fetches = ahead_of(ahead, near, ahead_sems)
    z, c = place[0], place[1]
    groups = sender.shape[0]
    n, _ = table_r.shape
    pair, regions = need.shape
    where_at = pieces_of(chips, offered)
    send = sender[...]
    remote, _, offset, _, _ = relative(send, n, pair, chips, z, c)
    position = iota((groups, 128), 0) * 128 + iota((groups, 128), 1)
    late = remote & jnp.logical_not(is_near(offset, chips)) & (position < live[0])
    late_bits = ones_where(late)
    within = dot(late_bits, ones_where(iota((128, 128), 0) < iota((128, 128), 1)))
    above = jnp.sum(dot(ones_where(iota((groups, groups), 1) < iota((groups, groups), 0)), late_bits), axis=1, keepdims=True)
    rank = jnp.where(late, (within + above).astype(I32), -1)
    total = jnp.sum(jnp.where(late, 1, 0))
    blocks = (total + LATE - 1) // LATE
    count[0] = blocks

    def one(block, carry):
        base = pl.multiple_of(block * LATE, LATE)
        lines = pl.ds(base, LATE)
        hot, send_at, receive_at = [], jnp.zeros((LATE, 128), I32), jnp.zeros((LATE, 128), I32)
        for g in range(groups):
            match = iota((LATE, 128), 0) + base == rank[g : g + 1, :]
            hot.append(ones_where(match))
            send_at += jnp.where(match, send[g : g + 1, :] + 1, 0)
            receive_at += jnp.where(match, receiver[g : g + 1, :] + 1, 0)
        edge = dot(jnp.concatenate(hot, axis=1), edges[...]).astype(BF)
        from_ = jnp.sum(send_at, axis=1, keepdims=True) - 1
        to = jnp.sum(receive_at, axis=1, keepdims=True) - 1
        valid, region, offset, half, slot = relative(from_, n, pair, chips, z, c)
        wanted = lax.dot_general(ones_where(iota((LATE, regions), 1) == region), need[...].astype(F32).astype(BF),
                                 (((1,), (1,)), ((), ())), preferred_element_type=F32)
        chosen = jnp.sum(jnp.where(iota((LATE, pair), 1) == slot, wanted, 0.0), axis=1, keepdims=True).astype(I32)
        start, flip = jnp.zeros((LATE, 1), I32), jnp.zeros((LATE, 1), I32)
        for key, (row, turned) in where_at.items():
            start = jnp.where(offset == key, row, start)
            flip = jnp.where(offset == key, turned, flip)
        at = jnp.where(valid, start + jnp.where(flip == 1, 1 - half, half) * offered + chosen, -1)
        rows[lines, :] = edge
        pre[lines, :] = dot(edge, w_e[...]) + dot(ones_where(iota((LATE, n), 1) == to), table_r[...])
        source_rows[lines, :] = gathered(at, sources, 0).astype(BF)
        at_out[lines, :] = jnp.broadcast_to(at, (LATE, 128))
        target_out[lines, :] = jnp.broadcast_to(to, (LATE, 128))
        return carry

    lax.fori_loop(0, blocks, one, 0)
    for fetch in fetches:
        fetch.wait()


def far_body(k, start, count, nodes, boundary, totals, bias, gain, node_bias, node_gain, w_s, w_out, node_in, node_out, *refs):
    m = AHEAD_GRID
    sources, (pre, rows, source_rows, at, target), ahead = refs[:k], refs[k : k + 5], refs[k + 5 : k + 5 + m]
    result, kept_result, published = refs[k + 5 + m : k + 8 + m]
    near, acc, ahead_sems = refs[k + 8 + m : k + 8 + 2 * m], refs[-2], refs[-1]
    n, f = nodes.shape
    fetches = ahead_of(ahead, near, ahead_sems)
    acc[...] = totals[...]

    def one(block, carry):
        lines = pl.ds(pl.multiple_of(block * LATE, LATE), LATE)
        source = (source_rows[lines, :].astype(F32) + gathered(at[lines, :][:, 0:1], sources, start)).astype(BF)
        update = finish(pre[lines, :] + dot(source, w_s[...]), bias[...], w_out[...], gain[...])
        message = (rows[lines, :].astype(F32) + update).astype(BF)
        eye = iota((128, 128), 0) == iota((128, 128), 1)
        targets = target[lines, :] + 1
        to = [jnp.sum(jnp.where(eye, targets[i : i + 128, :], 0), axis=0, keepdims=True) for i in range(0, LATE, 128)]
        acc[...] += dot(ones_where(iota((n, LATE), 0) + 1 == jnp.concatenate(to, axis=1)), message)
        return carry

    lax.fori_loop(0, count[0], one, 0)
    pre_node = dot(nodes[...], node_in[0:f, :]) + dot(acc[...].astype(BF), node_in[f : 2 * f, :])
    update = finish(pre_node, node_bias[...], node_out[...], node_gain[...])
    value = (nodes[...].astype(F32) + update).astype(BF)
    result[...] = value
    kept_result[...] = value
    hot = ones_where(iota((n, boundary.shape[1]), 0) == boundary[...])
    published[...] = dot_t(hot, value).astype(BF)
    for copy in fetches:
        copy.wait()


def grid_local_body(sender, mesh_out, w_s, before, out, table):
    n = mesh_out.shape[0]

    @pl.when(pl.program_id(0) == 0)
    def _():
        table[...] = dot(mesh_out[...], w_s[...]).astype(BF)

    out[...] = before[...] + dot(rows_hot(sender[0], n), table[...])


def grid_body(mesh_count, pair, sender, receiver_row, wanted, a, b, c, d, w_s, nodes, edges, before, bias, w_out, gain,
              node_in, node_bias, node_out, node_gain, result, totals, table):
    n, f = nodes.shape
    step = pl.program_id(0)
    rows = edges.shape[0]

    @pl.when(step == 0)
    def _():
        pieces = []
        for j, block in enumerate((a, b, c, d)):
            hot = ones_where(iota((block.shape[0], pair), 0) == wanted[j : j + 1, :])
            pieces.append(dot_t(hot, block[...]))
        chosen = jnp.concatenate(pieces, axis=0).astype(BF)
        table[...] = dot(chosen, w_s[...]).astype(BF)

    pre = before[...] + dot(rows_hot(sender[0] - mesh_count, table.shape[0]), table[...])
    update = finish(pre, bias[...], w_out[...], gain[...])
    message = (edges[...].astype(F32) + update).astype(BF)
    part = dot(ones_where(iota((n, rows), 0) == receiver_row[0]), message)

    @pl.when(step == 0)
    def _():
        totals[...] = part

    @pl.when(step > 0)
    def _():
        totals[...] += part

    @pl.when(step == pl.num_programs(0) - 1)
    def _():
        summed = totals[...].astype(BF)
        pre = dot(nodes[...], node_in[0:f, :]) + dot(summed, node_in[f : 2 * f, :])
        update = finish(pre, node_bias[...], node_out[...], node_gain[...])
        result[...] = (nodes[...].astype(F32) + update).astype(BF)


def local(
    mesh_nodes,
    mesh_edges,
    grid_nodes,
    grid_edges,
    boundary,
    mesh_need,
    mesh_sender,
    mesh_receiver,
    mesh_live,
    grid_need,
    grid_sender,
    grid_receiver,
    process_edge_in,
    process_edge_bias,
    process_edge_out,
    process_edge_gain,
    process_node_in,
    process_node_bias,
    process_node_out,
    process_node_gain,
    decode_edge_in,
    decode_edge_bias,
    decode_edge_out,
    decode_edge_gain,
    decode_node_in,
    decode_node_bias,
    decode_node_out,
    decode_node_gain,
):
    chips = lax.axis_size("z")
    regions = 2 * chips
    place = jnp.stack([lax.axis_index("z"), lax.axis_index("core")]).astype(I32)
    n, f = mesh_nodes.shape
    edges = mesh_edges.shape[0]
    grid_n = grid_nodes.shape[0]
    grid_e = grid_edges.shape[0]
    offered = boundary.shape[1]
    pair = mesh_need.shape[2]
    smem = pl.BlockSpec(memory_space=pltpu.SMEM)
    row = lambda v: v.reshape(1, -1)
    mesh_steps = edges // BLOCK
    grid_steps = grid_e // GRID_BLOCK
    as_blocks = lambda v, b: v.reshape(-1, b // 128, 128)
    as_rows = lambda v, b: v.reshape(-1, 1, b)
    idx_spec = lambda b: pl.BlockSpec((1, b // 128, 128), lambda i: (i, 0, 0))
    row_spec = lambda b: pl.BlockSpec((1, 1, b), lambda i: (i, 0, 0))
    tile = lambda b: pl.BlockSpec((b, f), lambda i: (i, 0))
    full = lambda v: (v, whole(v.shape))
    held = lambda v: (v, whole(v.shape), True)

    def along(steps):
        pairs = []
        for z in range(chips):
            pairs.append((2 * z, 2 * ((z + steps) % chips)))
            pairs.append((2 * z + 1, 2 * ((z - steps) % chips) + 1))
        return pairs

    def shift(v, steps):
        return lax.ppermute(v, REGION, along(steps))

    def swap(v):
        return lax.ppermute(v, "core", [(0, 1), (1, 0)])

    hbm = pl.BlockSpec(memory_space=HBM)
    anywhere = pl.BlockSpec(memory_space=pl.ANY)
    need = jnp.transpose(mesh_need[0])
    send_rows = mesh_sender.reshape(-1, 128)
    receive_rows = mesh_receiver.reshape(-1, 128)

    (own,) = call(publish_body, (1,), [(boundary, hbm), (mesh_nodes, hbm)], [((offered, f), BF, whole((offered, f)))],
                  [pltpu.VMEM((1, offered), I32), pltpu.VMEM((n, f), BF), pltpu.SemaphoreType.DMA((2,))],
                  flops=2 * offered * n * f, nbytes=2 * n * f)
    both = jnp.concatenate([own, swap(own)], axis=0)
    lead = [both]
    lead.append(shift(both, 1))
    seed = shift(both, SEED)
    for _ in range(2, REACH + 1):
        lead.append(shift(lead[-1], 1))
    back = [None]
    for k in range(1, REACH + 1):
        back.append(swap(lead[k]))
    seed_back = swap(seed)
    vmem = lambda v: ((f if v is decode_edge_in else v.shape[0], f), v.dtype, pl.BlockSpec(memory_space=VMEM), VMEM)
    mesh_needs = [process_edge_in, mesh_nodes, mesh_edges, process_edge_out]
    grid_before, w_in_near, nodes_near, edges_near, out_near = call(
        grid_before_body, (grid_steps,),
        [(as_rows(grid_receiver, GRID_BLOCK), row_spec(GRID_BLOCK)), full(grid_nodes), full(decode_edge_in),
         (grid_edges, tile(GRID_BLOCK)), (lead[1], anywhere)] + [(v, hbm) for v in mesh_needs],
        [((grid_e, f), F32, tile(GRID_BLOCK), HBM)] + [vmem(v) for v in mesh_needs],
        [pltpu.VMEM((grid_n, f), BF), pltpu.SemaphoreType.DMA((AHEAD_MESH,))],
        flops=2 * f * f * (grid_e * 2 + grid_n), nbytes=6 * grid_e * f,
    )
    before, table_r = call(
        before_body, (mesh_steps,),
        [(as_blocks(mesh_sender, BLOCK), idx_spec(BLOCK)), (as_blocks(mesh_receiver, BLOCK), idx_spec(BLOCK)), held(nodes_near),
         held(w_in_near), (edges_near, tile(BLOCK), True), (lead[2], anywhere)],
        [((edges, f), F32, tile(BLOCK), VMEM), ((n, f), BF, whole((n, f)), VMEM)],
        [pltpu.VMEM((n, f), BF)],
        flops=2 * f * f * (edges * 3 + 2 * n), nbytes=6 * edges * f,
    )
    halves = mesh_steps // 2
    ready = lead[3]
    current = jnp.concatenate([seed, seed_back], axis=0)
    chain, turned = [current], []
    for _ in range(STEPS):
        chain.append(shift(chain[-1], 1))
        turned.append(swap(chain[-1]))
    for part in range(2):
        first = part * halves
        at = lambda spec_rows, rank: pl.BlockSpec((1,) + spec_rows, lambda i: (i + first,) + (0,) * rank)
        moved = pl.BlockSpec((BLOCK, f), lambda i: (i + first, 0))
        (totals,) = call(
            functools.partial(main_body, chips, first), (halves,),
            [(place, smem), (mesh_live, smem), (as_blocks(mesh_sender, BLOCK), at((BLOCK // 128, 128), 2)),
             (as_rows(mesh_sender, BLOCK), at((1, BLOCK), 2)), (as_rows(mesh_receiver, BLOCK), at((1, BLOCK), 2)), full(need),
             (w_in_near, whole((f, f)), True), held(lead[0]), held(lead[1]), held(back[1]), (edges_near, moved, True),
             (before, moved, True), full(row(process_edge_bias)), held(out_near), full(row(process_edge_gain)),
             (ready, anywhere)] + ([held(totals)] if part else []),
            [((n, f), F32, whole((n, f)), VMEM)],
            [pltpu.VMEM((6 * pair, f), BF)],
            flops=2 * f * f * halves * BLOCK * 2, nbytes=6 * halves * BLOCK * f,
        )
        ready = lead[4]
    arrays = {"lead": lead, "back": back, "chain": chain, "turn": turned}
    early, last = [[arrays[kind][k] for (kind, k), _ in part] for part in layout()]
    early_rows = sum(v.shape[0] for v in early)
    far_needs = [process_node_in, process_node_out]
    grid_needs = [grid_before, decode_edge_in, grid_nodes, grid_edges, decode_edge_out, decode_node_in, decode_node_out]
    on_chip = lambda dtype, width: ((edges, width), dtype, pl.BlockSpec(memory_space=VMEM), VMEM)
    *stored, count, node_in_near, node_out_near = call(
        functools.partial(compact_body, chips, offered, len(early)), (1,),
        [(place, smem), (mesh_live, smem), full(send_rows), full(receive_rows), full(need),
         (w_in_near, pl.BlockSpec((f, f), lambda i: (2, 0)), True), held(table_r), held(edges_near)]
        + [held(v) for v in early] + [(v, hbm) for v in far_needs],
        [on_chip(F32, f), on_chip(BF, f), on_chip(BF, f), on_chip(I32, 128), on_chip(I32, 128), ((1,), I32, smem)]
        + [vmem(v) for v in far_needs],
        [pltpu.SemaphoreType.DMA((AHEAD_FAR,))],
        flops=2 * f * 128 * (edges + 4 * f), nbytes=2 * edges * f,
    )
    mesh_out, mesh_kept, published, grid_before, grid_head, nodes_g, edges_g, out_g, node_in_g, node_out_g = call(
        functools.partial(far_body, len(last), early_rows), (1,),
        [(count, smem), held(nodes_near), full(boundary), held(totals), full(row(process_edge_bias)),
         full(row(process_edge_gain)), full(row(process_node_bias)), full(row(process_node_gain)), (w_in_near, whole((f, f)), True),
         held(out_near), held(node_in_near), held(node_out_near)] + [held(v) for v in last]
        + [(v, pl.BlockSpec(memory_space=VMEM), True) for v in stored] + [(v, hbm) for v in grid_needs],
        [((n, f), BF, whole((n, f))), ((n, f), BF, whole((n, f)), VMEM), ((offered, f), BF, whole((offered, f)), VMEM)]
        + [vmem(v) for v in grid_needs],
        [pltpu.VMEM((n, f), F32), pltpu.SemaphoreType.DMA((AHEAD_GRID,))],
        flops=2 * f * f * 4 * n, nbytes=8 * n * f,
    )
    pieces = []
    for offset in (-2, -1, 1, 2):
        pieces.append(lax.ppermute(published, REGION, [(s, (s - offset) % regions) for s in range(regions)]))
    (grid_local,) = call(
        grid_local_body, (grid_steps,),
        [(as_rows(grid_sender, GRID_BLOCK), row_spec(GRID_BLOCK)), held(mesh_kept), held(grid_head),
         (grid_before, tile(GRID_BLOCK), True)],
        [((grid_e, f), F32, tile(GRID_BLOCK), VMEM)],
        [pltpu.VMEM((n, f), BF)],
        flops=2 * f * f * (grid_e + n), nbytes=8 * grid_e * f,
    )
    (grid_out,) = call(
        functools.partial(grid_body, n, pair), (grid_steps,),
        [(as_rows(grid_sender, GRID_BLOCK), row_spec(GRID_BLOCK)), (as_rows(grid_receiver, GRID_BLOCK), row_spec(GRID_BLOCK)),
         full(grid_need[0]), held(pieces[0]), held(pieces[1]), held(pieces[2]), held(pieces[3]),
         held(grid_head), held(nodes_g), (edges_g, tile(GRID_BLOCK), True), (grid_local, tile(GRID_BLOCK), True),
         full(row(decode_edge_bias)), held(out_g), full(row(decode_edge_gain)), held(node_in_g),
         full(row(decode_node_bias)), held(node_out_g), full(row(decode_node_gain))],
        [((grid_n, f), BF, whole((grid_n, f)))],
        [pltpu.VMEM((grid_n, f), F32), pltpu.VMEM((4 * pair, f), BF)],
        flops=2 * f * f * (grid_e * 2 + 3 * grid_n), nbytes=6 * grid_e * f,
    )
    return (mesh_out, grid_out)


def solution(mesh):
    cores = 2
    finer = Mesh(
        mesh.devices.reshape(mesh.shape["member"], mesh.shape["region"] // cores, cores), ("member", "z", "core")
    )
    in_specs = (
        P(MEMBER_REGION, None),
        P(REGION, None),
        P(MEMBER_REGION, None),
        P(REGION, None),
        P(REGION, None),
        P(REGION, None, None),
        P(REGION, None),
        P(REGION, None),
        P(REGION),
        P(REGION, None, None),
        P(REGION, None),
        P(REGION, None),
    ) + (P(),) * 16
    out_specs = (P(MEMBER_REGION, None), P(MEMBER_REGION, None))

    return jax.shard_map(local, mesh=finer, in_specs=in_specs, out_specs=out_specs, check_vma=False)
```

```python
import functools

import jax
import jax.numpy as jnp
from jax import lax
from jax.experimental import pallas as pl
from jax.experimental.pallas import tpu as pltpu
from jax.sharding import Mesh
from jax.sharding import PartitionSpec as P

REGION = ("z", "core")
MEMBER_REGION = ("member", "z", "core")
BF = jnp.bfloat16
F32 = jnp.float32
I32 = jnp.int32
HBM = pltpu.MemorySpace.HBM
VMEM = pltpu.MemorySpace.VMEM
SEED = 12
LEAD = 3
STEPS = 4
LATE = 256
AHEAD_MESH = 4
AHEAD_FAR = 2
AHEAD_GRID = 7
BLOCK = 512
GRID_BLOCK = 384
LIMIT = 24 * 2**20


def iota(shape, dim):
    return lax.broadcasted_iota(I32, shape, dim)


def ones_where(mask):
    return jnp.where(mask, 1.0, 0.0).astype(BF)


def dot(a, b):
    return jnp.dot(a, b, preferred_element_type=F32)


def dot_t(a, b):
    return lax.dot_general(a, b, (((0,), (0,)), ((), ())), preferred_element_type=F32)


def columns(rows):
    lines = [rows[i : i + 1, j : j + 128] for i in range(rows.shape[0]) for j in range(0, rows.shape[1], 128)]
    eye = iota((128, 128), 0) == iota((128, 128), 1)
    return [jnp.sum(jnp.where(eye, jnp.broadcast_to(line, (128, 128)), 0), axis=1, keepdims=True) for line in lines]


def rows_hot(rows, count):
    return jnp.concatenate([ones_where(iota((128, count), 1) == c) for c in columns(rows)], axis=0)


def silu(x):
    half = 0.5 * x
    return half + half * jnp.tanh(half)


def finish(pre, bias, w_out, gain):
    hidden = silu(pre + bias).astype(BF)
    y = dot(hidden, w_out)
    y = y - jnp.mean(y, axis=1, keepdims=True)
    spread = jnp.mean(y * y, axis=1, keepdims=True)
    return y * lax.rsqrt(spread + 0.25) * gain


def whole(shape):
    return pl.BlockSpec(shape, lambda *_: (0,) * len(shape))


def call(body, grid, ins, outs, scratch=(), flops=0, nbytes=0):
    place = lambda a, s, *near: a if near or s.memory_space not in (None, HBM) else pltpu.with_memory_space_constraint(a, HBM)
    result = lambda s, d, p, *at: at[0](s, d) if at else HBM(s, d) if p.memory_space == HBM else jax.ShapeDtypeStruct(s, d)
    return pl.pallas_call(
        body,
        grid=grid,
        in_specs=[i[1] for i in ins],
        out_specs=[o[2] for o in outs],
        out_shape=[result(*o) for o in outs],
        scratch_shapes=list(scratch),
        compiler_params=pltpu.CompilerParams(vmem_limit_bytes=LIMIT),
        cost_estimate=pl.CostEstimate(flops=flops, bytes_accessed=nbytes, transcendentals=0),
    )(*[place(*i) for i in ins])


def publish_body(boundary_hbm, nodes_hbm, out, boundary, nodes, sems):
    copies = [pltpu.make_async_copy(boundary_hbm, boundary, sems.at[0]), pltpu.make_async_copy(nodes_hbm, nodes, sems.at[1])]
    for copy in copies:
        copy.start()
    for copy in copies:
        copy.wait()
    hot = ones_where(iota((nodes.shape[0], boundary.shape[1]), 0) == boundary[...])
    out[...] = dot_t(hot, nodes[...]).astype(BF)


def before_body(sender, receiver, nodes, w_in, edges, ready, out, table_r, table_s):
    n, f = nodes.shape

    @pl.when(pl.program_id(0) == 0)
    def _():
        table_s[...] = dot(nodes[...], w_in[0:f, :]).astype(BF)
        table_r[...] = dot(nodes[...], w_in[f : 2 * f, :]).astype(BF)

    total = dot(edges[...], w_in[2 * f : 3 * f, :])
    total += dot(rows_hot(sender[0], n), table_s[...])
    total += dot(rows_hot(receiver[0], n), table_r[...])
    out[...] = total


def grid_before_body(receiver, nodes, w_in, edges, ready, *refs):
    m = AHEAD_MESH
    ahead, out, near, table_r, sems = refs[:m], refs[m], refs[m + 1 : 2 * m + 1], refs[-2], refs[-1]
    n, f = nodes.shape

    @pl.when(pl.program_id(0) == 0)
    def _():
        ahead_of(ahead, near, sems)
        table_r[...] = dot(nodes[...], w_in[f : 2 * f, :]).astype(BF)

    out[...] = dot(edges[...], w_in[2 * f : 3 * f, :]) + dot(rows_hot(receiver[0], n), table_r[...])

    @pl.when(pl.program_id(0) == pl.num_programs(0) - 1)
    def _():
        for copy in ahead_of(ahead, near, sems, False):
            copy.wait()


def pieces_of(chips, offered):
    pair = 2 * offered
    far = [(2, 0), (-2, 1)]
    for step in range(STEPS + 1):
        far += [(LEAD + step, 0), (SEED + step, 0), (step - SEED, 1)]
    far += [(-LEAD, 1)]
    for step in range(1, STEPS + 1):
        far += [(-LEAD - step, 1), (-SEED - step, 1), (SEED - step, 0)]
    table = {}
    for i, (offset, flip) in enumerate(far):
        table.setdefault(offset % chips, (i * pair, flip))
    return table


def relative(sender, n, pair, chips, z, c):
    far = sender - n
    region = far // pair
    sign = 2 * c - 1
    offset = (sign * (region // 2 - z) + 2 * chips) % chips
    half = jnp.where(region % 2 == c, 0, 1)
    return far >= 0, region, offset, half, far % pair


def is_near(offset, chips):
    return (offset <= 1) | (offset == chips - 1)


def main_body(chips, first, place, live, sender, sender_row, receiver_row, need, w_s, both, up, down, edges, before, bias, w_out,
              gain, ready, *refs):
    totals, table = refs[-2:]
    z, c = place[0], place[1]
    n, _ = totals.shape
    step = pl.program_id(0)
    rows = edges.shape[0]
    pair, regions = need.shape
    offered = both.shape[0] // 2

    @pl.when(step == 0)
    def _():
        totals[...] = refs[0][...] if first else jnp.zeros_like(totals)
        r = iota((6 * pair, regions), 0)
        near = r // (2 * pair)
        half = (r // pair) % 2
        moved = jnp.where(near == 2, -1, near)
        chip = (z + (2 * c - 1) * moved + chips) % chips
        region = 2 * chip + jnp.where(half == 1, 1 - c, c)
        wanted = lax.dot_general(ones_where(iota((6 * pair, regions), 1) == region), need[...].astype(F32).astype(BF),
                                 (((1,), (1,)), ((), ())), preferred_element_type=F32)
        lane = iota((6 * pair, pair), 1) == iota((6 * pair, pair), 0) % pair
        column = jnp.sum(jnp.where(lane, wanted, 0.0), axis=1, keepdims=True).astype(I32)
        chosen = []
        for j, (source, flip) in enumerate(((both, 0), (up, 0), (down, 1))):
            own_half = iota((2 * pair, 2 * offered), 0) // pair
            at = (1 - own_half if flip else own_half) * offered + column[j * 2 * pair : (j + 1) * 2 * pair, :]
            chosen.append(dot(ones_where(iota((2 * pair, 2 * offered), 1) == at), source[...]))
        table[...] = dot(jnp.concatenate(chosen, axis=0).astype(BF), w_s[...]).astype(BF)

    remote, _, offset, half, slot = relative(sender[0], n, pair, chips, z, c)
    near = jnp.where(offset == chips - 1, 2, offset)
    place_of = jnp.where(remote & is_near(offset, chips), near * 2 * pair + half * pair + slot, -1)
    pre = before[...] + dot(rows_hot(place_of, 6 * pair), table[...])
    update = finish(pre, bias[...], w_out[...], gain[...])
    message = (edges[...].astype(F32) + update).astype(BF)
    position = (first + step) * rows + iota((1, rows), 1)
    remote, _, offset, _, _ = relative(sender_row[0], n, pair, chips, z, c)
    later = remote & jnp.logical_not(is_near(offset, chips))
    target = jnp.where((position < live[0]) & jnp.logical_not(later), receiver_row[0], -1)
    totals[...] += dot(ones_where(iota((n, rows), 0) == target), message)


def ahead_of(sources, targets, sems, begin=True):
    copies = [pltpu.make_async_copy(a.at[pl.ds(0, b.shape[0]), :], b, sems.at[i]) for i, (a, b) in enumerate(zip(sources, targets))]
    for copy in copies if begin else ():
        copy.start()
    return copies


def gathered(at, sources, starts):
    out = None
    for source, start in zip(sources, starts):
        hot = ones_where(iota((at.shape[0], source.shape[0]), 1) + start == at)
        part = dot(hot, source[...])
        out = part if out is None else out + part
    return out


def compact_body(chips, offered, starts, place, live, sender, receiver, need, w_e, table_r, edges, *refs):
    k, m = len(starts), AHEAD_FAR
    sources, ahead = refs[:k], refs[k : k + m]
    outs, count, near = refs[k + m : k + m + 5], refs[k + m + 5], refs[k + m + 6 : k + 2 * m + 6]
    ahead_sems = refs[-1]
    pre, rows, source_rows, at_out, target_out = outs
    fetches = ahead_of(ahead, near, ahead_sems)
    z, c = place[0], place[1]
    groups = sender.shape[0]
    n, _ = table_r.shape
    pair, regions = need.shape
    where_at = pieces_of(chips, offered)
    send = sender[...]
    remote, _, offset, _, _ = relative(send, n, pair, chips, z, c)
    position = iota((groups, 128), 0) * 128 + iota((groups, 128), 1)
    late = remote & jnp.logical_not(is_near(offset, chips)) & (position < live[0])
    late_bits = ones_where(late)
    within = dot(late_bits, ones_where(iota((128, 128), 0) < iota((128, 128), 1)))
    above = jnp.sum(dot(ones_where(iota((groups, groups), 1) < iota((groups, groups), 0)), late_bits), axis=1, keepdims=True)
    rank = jnp.where(late, (within + above).astype(I32), -1)
    total = jnp.sum(jnp.where(late, 1, 0))
    blocks = (total + LATE - 1) // LATE
    count[0] = blocks

    def one(block, carry):
        base = pl.multiple_of(block * LATE, LATE)
        lines = pl.ds(base, LATE)
        hot, send_at, receive_at = [], jnp.zeros((LATE, 128), I32), jnp.zeros((LATE, 128), I32)
        for g in range(groups):
            match = iota((LATE, 128), 0) + base == rank[g : g + 1, :]
            hot.append(ones_where(match))
            send_at += jnp.where(match, send[g : g + 1, :] + 1, 0)
            receive_at += jnp.where(match, receiver[g : g + 1, :] + 1, 0)
        edge = dot(jnp.concatenate(hot, axis=1), edges[...]).astype(BF)
        from_ = jnp.sum(send_at, axis=1, keepdims=True) - 1
        to = jnp.sum(receive_at, axis=1, keepdims=True) - 1
        valid, region, offset, half, slot = relative(from_, n, pair, chips, z, c)
        wanted = lax.dot_general(ones_where(iota((LATE, regions), 1) == region), need[...].astype(F32).astype(BF),
                                 (((1,), (1,)), ((), ())), preferred_element_type=F32)
        chosen = jnp.sum(jnp.where(iota((LATE, pair), 1) == slot, wanted, 0.0), axis=1, keepdims=True).astype(I32)
        start, flip = jnp.zeros((LATE, 1), I32), jnp.zeros((LATE, 1), I32)
        for key, (row, turned) in where_at.items():
            start = jnp.where(offset == key, row, start)
            flip = jnp.where(offset == key, turned, flip)
        at = jnp.where(valid, start + jnp.where(flip == 1, 1 - half, half) * offered + chosen, -1)
        rows[lines, :] = edge
        pre[lines, :] = dot(edge, w_e[...]) + dot(ones_where(iota((LATE, n), 1) == to), table_r[...])
        source_rows[lines, :] = gathered(at, sources, starts).astype(BF)
        at_out[lines, :] = jnp.broadcast_to(at, (LATE, 128))
        target_out[lines, :] = jnp.broadcast_to(to, (LATE, 128))
        return carry

    lax.fori_loop(0, blocks, one, 0)
    for fetch in fetches:
        fetch.wait()


def node_part_body(nodes, w_in, grid_nodes, grid_w_in, ready, out, grid_out):
    out[...] = dot(nodes[...], w_in[...])
    grid_out[...] = dot(grid_nodes[...], grid_w_in[...])


def far_body(starts, count, nodes, node_part, boundary, totals, bias, gain, node_bias, node_gain, w_s, w_out, node_in, node_out, *refs):
    k, m = len(starts), AHEAD_GRID
    sources, (pre, rows, source_rows, at, target), ahead = refs[:k], refs[k : k + 5], refs[k + 5 : k + 5 + m]
    result, kept_result, published = refs[k + 5 + m : k + 8 + m]
    near, acc, ahead_sems = refs[k + 8 + m : k + 8 + 2 * m], refs[-2], refs[-1]
    n, f = nodes.shape
    fetches = ahead_of(ahead, near, ahead_sems)
    acc[...] = totals[...]

    def one(block, carry):
        lines = pl.ds(pl.multiple_of(block * LATE, LATE), LATE)
        source = (source_rows[lines, :].astype(F32) + gathered(at[lines, :][:, 0:1], sources, starts)).astype(BF)
        update = finish(pre[lines, :] + dot(source, w_s[...]), bias[...], w_out[...], gain[...])
        message = (rows[lines, :].astype(F32) + update).astype(BF)
        eye = iota((128, 128), 0) == iota((128, 128), 1)
        targets = target[lines, :] + 1
        to = [jnp.sum(jnp.where(eye, targets[i : i + 128, :], 0), axis=0, keepdims=True) for i in range(0, LATE, 128)]
        acc[...] += dot(ones_where(iota((n, LATE), 0) + 1 == jnp.concatenate(to, axis=1)), message)
        return carry

    lax.fori_loop(0, count[0], one, 0)
    pre_node = node_part[...] + dot(acc[...].astype(BF), node_in[f : 2 * f, :])
    update = finish(pre_node, node_bias[...], node_out[...], node_gain[...])
    value = (nodes[...].astype(F32) + update).astype(BF)
    result[...] = value
    kept_result[...] = value
    hot = ones_where(iota((n, boundary.shape[1]), 0) == boundary[...])
    published[...] = dot_t(hot, value).astype(BF)
    for copy in fetches:
        copy.wait()


def grid_local_body(sender, mesh_out, w_s, before, out, table):
    n = mesh_out.shape[0]

    @pl.when(pl.program_id(0) == 0)
    def _():
        table[...] = dot(mesh_out[...], w_s[...]).astype(BF)

    out[...] = before[...] + dot(rows_hot(sender[0], n), table[...])


def grid_body(mesh_count, pair, sender, receiver_row, wanted, a, b, c, d, w_s, nodes, node_part, edges, before, bias, w_out, gain,
              node_in, node_bias, node_out, node_gain, result, totals, table):
    n, f = nodes.shape
    step = pl.program_id(0)
    rows = edges.shape[0]

    @pl.when(step == 0)
    def _():
        pieces = []
        for j, block in enumerate((a, b, c, d)):
            hot = ones_where(iota((block.shape[0], pair), 0) == wanted[j : j + 1, :])
            pieces.append(dot_t(hot, block[...]))
        chosen = jnp.concatenate(pieces, axis=0).astype(BF)
        table[...] = dot(chosen, w_s[...]).astype(BF)

    pre = before[...] + dot(rows_hot(sender[0] - mesh_count, table.shape[0]), table[...])
    update = finish(pre, bias[...], w_out[...], gain[...])
    message = (edges[...].astype(F32) + update).astype(BF)
    part = dot(ones_where(iota((n, rows), 0) == receiver_row[0]), message)

    @pl.when(step == 0)
    def _():
        totals[...] = part

    @pl.when(step > 0)
    def _():
        totals[...] += part

    @pl.when(step == pl.num_programs(0) - 1)
    def _():
        summed = totals[...].astype(BF)
        pre = node_part[...] + dot(summed, node_in[f : 2 * f, :])
        update = finish(pre, node_bias[...], node_out[...], node_gain[...])
        result[...] = (nodes[...].astype(F32) + update).astype(BF)


def local(
    mesh_nodes,
    mesh_edges,
    grid_nodes,
    grid_edges,
    boundary,
    mesh_need,
    mesh_sender,
    mesh_receiver,
    mesh_live,
    grid_need,
    grid_sender,
    grid_receiver,
    process_edge_in,
    process_edge_bias,
    process_edge_out,
    process_edge_gain,
    process_node_in,
    process_node_bias,
    process_node_out,
    process_node_gain,
    decode_edge_in,
    decode_edge_bias,
    decode_edge_out,
    decode_edge_gain,
    decode_node_in,
    decode_node_bias,
    decode_node_out,
    decode_node_gain,
):
    chips = lax.axis_size("z")
    regions = 2 * chips
    place = jnp.stack([lax.axis_index("z"), lax.axis_index("core")]).astype(I32)
    n, f = mesh_nodes.shape
    edges = mesh_edges.shape[0]
    grid_n = grid_nodes.shape[0]
    grid_e = grid_edges.shape[0]
    offered = boundary.shape[1]
    pair = mesh_need.shape[2]
    smem = pl.BlockSpec(memory_space=pltpu.SMEM)
    row = lambda v: v.reshape(1, -1)
    mesh_steps = edges // BLOCK
    grid_steps = grid_e // GRID_BLOCK
    as_blocks = lambda v, b: v.reshape(-1, b // 128, 128)
    as_rows = lambda v, b: v.reshape(-1, 1, b)
    idx_spec = lambda b: pl.BlockSpec((1, b // 128, 128), lambda i: (i, 0, 0))
    row_spec = lambda b: pl.BlockSpec((1, 1, b), lambda i: (i, 0, 0))
    tile = lambda b: pl.BlockSpec((b, f), lambda i: (i, 0))
    full = lambda v: (v, whole(v.shape))
    held = lambda v: (v, whole(v.shape), True)

    def along(steps):
        pairs = []
        for z in range(chips):
            pairs.append((2 * z, 2 * ((z + steps) % chips)))
            pairs.append((2 * z + 1, 2 * ((z - steps) % chips) + 1))
        return pairs

    def shift(v, steps):
        return lax.ppermute(v, REGION, along(steps))

    def swap(v):
        return lax.ppermute(v, "core", [(0, 1), (1, 0)])

    hbm = pl.BlockSpec(memory_space=HBM)
    anywhere = pl.BlockSpec(memory_space=pl.ANY)
    need = jnp.transpose(mesh_need[0])
    send_rows = mesh_sender.reshape(-1, 128)
    receive_rows = mesh_receiver.reshape(-1, 128)

    (own,) = call(publish_body, (1,), [(boundary, hbm), (mesh_nodes, hbm)], [((offered, f), BF, whole((offered, f)))],
                  [pltpu.VMEM((1, offered), I32), pltpu.VMEM((n, f), BF), pltpu.SemaphoreType.DMA((2,))],
                  flops=2 * offered * n * f, nbytes=2 * n * f)
    both = jnp.concatenate([own, swap(own)], axis=0)
    lead = [both]
    lead.append(shift(both, 1))
    seed = shift(both, SEED)
    lead.append(shift(lead[1], 1))
    lead.append(shift(lead[2], 1))
    back = [None]
    for k in range(1, LEAD + 1):
        back.append(swap(lead[k]))
    seed_back = swap(seed)
    vmem = lambda v: ((f if v is decode_edge_in else v.shape[0], f), v.dtype, pl.BlockSpec(memory_space=VMEM), VMEM)
    mesh_needs = [process_edge_in, mesh_nodes, mesh_edges, process_edge_out]
    grid_before, w_in_near, nodes_near, edges_near, out_near = call(
        grid_before_body, (grid_steps,),
        [(as_rows(grid_receiver, GRID_BLOCK), row_spec(GRID_BLOCK)), full(grid_nodes), full(decode_edge_in),
         (grid_edges, tile(GRID_BLOCK)), (lead[1], anywhere)] + [(v, hbm) for v in mesh_needs],
        [((grid_e, f), F32, tile(GRID_BLOCK), HBM)] + [vmem(v) for v in mesh_needs],
        [pltpu.VMEM((grid_n, f), BF), pltpu.SemaphoreType.DMA((AHEAD_MESH,))],
        flops=2 * f * f * (grid_e * 2 + grid_n), nbytes=6 * grid_e * f,
    )
    before, table_r = call(
        before_body, (mesh_steps,),
        [(as_blocks(mesh_sender, BLOCK), idx_spec(BLOCK)), (as_blocks(mesh_receiver, BLOCK), idx_spec(BLOCK)), held(nodes_near),
         held(w_in_near), (edges_near, tile(BLOCK), True), (lead[2], anywhere)],
        [((edges, f), F32, tile(BLOCK), VMEM), ((n, f), BF, whole((n, f)), VMEM)],
        [pltpu.VMEM((n, f), BF)],
        flops=2 * f * f * (edges * 3 + 2 * n), nbytes=6 * edges * f,
    )
    halves = mesh_steps // 2
    ready = lead[3]
    current = jnp.concatenate([lead[3], seed, seed_back], axis=0)
    chain, turned = [current], []
    for _ in range(STEPS):
        chain.append(shift(chain[-1], 1))
        turned.append(swap(chain[-1]))
    for part in range(2):
        first = part * halves
        at = lambda spec_rows, rank: pl.BlockSpec((1,) + spec_rows, lambda i: (i + first,) + (0,) * rank)
        moved = pl.BlockSpec((BLOCK, f), lambda i: (i + first, 0))
        (totals,) = call(
            functools.partial(main_body, chips, first), (halves,),
            [(place, smem), (mesh_live, smem), (as_blocks(mesh_sender, BLOCK), at((BLOCK // 128, 128), 2)),
             (as_rows(mesh_sender, BLOCK), at((1, BLOCK), 2)), (as_rows(mesh_receiver, BLOCK), at((1, BLOCK), 2)), full(need),
             (w_in_near, whole((f, f)), True), held(lead[0]), held(lead[1]), held(back[1]), (edges_near, moved, True),
             (before, moved, True), full(row(process_edge_bias)), held(out_near), full(row(process_edge_gain)),
             (ready, anywhere)] + ([held(totals)] if part else []),
            [((n, f), F32, whole((n, f)), VMEM)],
            [pltpu.VMEM((6 * pair, f), BF)],
            flops=2 * f * f * halves * BLOCK * 2, nbytes=6 * halves * BLOCK * f,
        )
        ready = chain[1]
    far = [lead[2], back[2]] + chain + [back[3]] + turned
    starts, at_row = [], 0
    for v in far:
        starts.append(at_row)
        at_row += v.shape[0]
    last = [STEPS + 2, len(far) - 2, len(far) - 1]
    early = [i for i in range(len(far)) if i not in last]
    far_needs = [process_node_in, process_node_out]
    grid_needs = [grid_before, decode_edge_in, grid_nodes, grid_edges, decode_edge_out, decode_node_in, decode_node_out]
    on_chip = lambda dtype, width: ((edges, width), dtype, pl.BlockSpec(memory_space=VMEM), VMEM)
    mesh_part, grid_part = call(
        node_part_body, (1,),
        [held(nodes_near), (process_node_in, whole((f, f))), full(grid_nodes), (decode_node_in, whole((f, f))),
         (chain[2], anywhere)],
        [((n, f), F32, whole((n, f)), VMEM), ((grid_n, f), F32, whole((grid_n, f)), VMEM)],
        flops=2 * f * f * (n + grid_n), nbytes=4 * n * f,
    )
    *stored, count, node_in_near, node_out_near = call(
        functools.partial(compact_body, chips, offered, tuple(starts[i] for i in early)), (1,),
        [(place, smem), (mesh_live, smem), full(send_rows), full(receive_rows), full(need),
         (w_in_near, pl.BlockSpec((f, f), lambda i: (2, 0)), True), held(table_r), held(edges_near)]
        + [held(far[i]) for i in early] + [(v, hbm) for v in far_needs],
        [on_chip(F32, f), on_chip(BF, f), on_chip(BF, f), on_chip(I32, 128), on_chip(I32, 128), ((1,), I32, smem)]
        + [vmem(v) for v in far_needs],
        [pltpu.SemaphoreType.DMA((AHEAD_FAR,))],
        flops=2 * f * 128 * (edges + 4 * f), nbytes=2 * edges * f,
    )
    mesh_out, mesh_kept, published, grid_before, grid_head, nodes_g, edges_g, out_g, node_in_g, node_out_g = call(
        functools.partial(far_body, tuple(starts[i] for i in last)), (1,),
        [(count, smem), held(nodes_near), held(mesh_part), full(boundary), held(totals), full(row(process_edge_bias)),
         full(row(process_edge_gain)), full(row(process_node_bias)), full(row(process_node_gain)), (w_in_near, whole((f, f)), True),
         held(out_near), held(node_in_near), held(node_out_near)] + [held(far[i]) for i in last]
        + [(v, pl.BlockSpec(memory_space=VMEM), True) for v in stored] + [(v, hbm) for v in grid_needs],
        [((n, f), BF, whole((n, f))), ((n, f), BF, whole((n, f)), VMEM), ((offered, f), BF, whole((offered, f)), VMEM)]
        + [vmem(v) for v in grid_needs],
        [pltpu.VMEM((n, f), F32), pltpu.SemaphoreType.DMA((AHEAD_GRID,))],
        flops=2 * f * f * 4 * n, nbytes=8 * n * f,
    )
    pieces = []
    for offset in (-2, -1, 1, 2):
        pieces.append(lax.ppermute(published, REGION, [(s, (s - offset) % regions) for s in range(regions)]))
    (grid_local,) = call(
        grid_local_body, (grid_steps,),
        [(as_rows(grid_sender, GRID_BLOCK), row_spec(GRID_BLOCK)), held(mesh_kept), held(grid_head),
         (grid_before, tile(GRID_BLOCK), True)],
        [((grid_e, f), F32, tile(GRID_BLOCK), VMEM)],
        [pltpu.VMEM((n, f), BF)],
        flops=2 * f * f * (grid_e + n), nbytes=8 * grid_e * f,
    )
    (grid_out,) = call(
        functools.partial(grid_body, n, pair), (grid_steps,),
        [(as_rows(grid_sender, GRID_BLOCK), row_spec(GRID_BLOCK)), (as_rows(grid_receiver, GRID_BLOCK), row_spec(GRID_BLOCK)),
         full(grid_need[0]), held(pieces[0]), held(pieces[1]), held(pieces[2]), held(pieces[3]),
         held(grid_head), held(nodes_g), held(grid_part), (edges_g, tile(GRID_BLOCK), True), (grid_local, tile(GRID_BLOCK), True),
         full(row(decode_edge_bias)), held(out_g), full(row(decode_edge_gain)), held(node_in_g),
         full(row(decode_node_bias)), held(node_out_g), full(row(decode_node_gain))],
        [((grid_n, f), BF, whole((grid_n, f)))],
        [pltpu.VMEM((grid_n, f), F32), pltpu.VMEM((4 * pair, f), BF)],
        flops=2 * f * f * (grid_e * 2 + 3 * grid_n), nbytes=6 * grid_e * f,
    )
    return (mesh_out, grid_out)


def solution(mesh):
    cores = 2
    finer = Mesh(
        mesh.devices.reshape(mesh.shape["member"], mesh.shape["region"] // cores, cores), ("member", "z", "core")
    )
    in_specs = (
        P(MEMBER_REGION, None),
        P(REGION, None),
        P(MEMBER_REGION, None),
        P(REGION, None),
        P(REGION, None),
        P(REGION, None, None),
        P(REGION, None),
        P(REGION, None),
        P(REGION),
        P(REGION, None, None),
        P(REGION, None),
        P(REGION, None),
    ) + (P(),) * 16
    out_specs = (P(MEMBER_REGION, None), P(MEMBER_REGION, None))

    return jax.shard_map(local, mesh=finer, in_specs=in_specs, out_specs=out_specs, check_vma=False)
```

```python
import functools

import jax
import jax.numpy as jnp
from jax import lax
from jax.experimental import pallas as pl
from jax.experimental.pallas import tpu as pltpu
from jax.sharding import Mesh
from jax.sharding import PartitionSpec as P

REGION = ("z", "core")
MEMBER_REGION = ("member", "z", "core")
BF = jnp.bfloat16
F32 = jnp.float32
I32 = jnp.int32
HBM = pltpu.MemorySpace.HBM
VMEM = pltpu.MemorySpace.VMEM
SEED = 12
LEAD = 3
STEPS = 4
LATE = 256
AHEAD_MESH = 4
AHEAD_FAR = 2
AHEAD_GRID = 7
BLOCK = 512
GRID_BLOCK = 384
LIMIT = 24 * 2**20


def iota(shape, dim):
    return lax.broadcasted_iota(I32, shape, dim)


def ones_where(mask):
    return jnp.where(mask, 1.0, 0.0).astype(BF)


def dot(a, b):
    return jnp.dot(a, b, preferred_element_type=F32)


def dot_t(a, b):
    return lax.dot_general(a, b, (((0,), (0,)), ((), ())), preferred_element_type=F32)


def columns(rows):
    lines = [rows[i : i + 1, j : j + 128] for i in range(rows.shape[0]) for j in range(0, rows.shape[1], 128)]
    eye = iota((128, 128), 0) == iota((128, 128), 1)
    return [jnp.sum(jnp.where(eye, jnp.broadcast_to(line, (128, 128)), 0), axis=1, keepdims=True) for line in lines]


def rows_hot(rows, count):
    return jnp.concatenate([ones_where(iota((128, count), 1) == c) for c in columns(rows)], axis=0)


def silu(x):
    half = 0.5 * x
    return half + half * jnp.tanh(half)


def finish(pre, bias, w_out, gain):
    hidden = silu(pre + bias).astype(BF)
    y = dot(hidden, w_out)
    y = y - jnp.mean(y, axis=1, keepdims=True)
    spread = jnp.mean(y * y, axis=1, keepdims=True)
    return y * lax.rsqrt(spread + 0.25) * gain


def whole(shape):
    return pl.BlockSpec(shape, lambda *_: (0,) * len(shape))


def call(body, grid, ins, outs, scratch=(), flops=0, nbytes=0):
    place = lambda a, s, *near: a if near or s.memory_space not in (None, HBM) else pltpu.with_memory_space_constraint(a, HBM)
    result = lambda s, d, p, *at: at[0](s, d) if at else HBM(s, d) if p.memory_space == HBM else jax.ShapeDtypeStruct(s, d)
    return pl.pallas_call(
        body,
        grid=grid,
        in_specs=[i[1] for i in ins],
        out_specs=[o[2] for o in outs],
        out_shape=[result(*o) for o in outs],
        scratch_shapes=list(scratch),
        compiler_params=pltpu.CompilerParams(vmem_limit_bytes=LIMIT),
        cost_estimate=pl.CostEstimate(flops=flops, bytes_accessed=nbytes, transcendentals=0),
    )(*[place(*i) for i in ins])


def publish_body(boundary_hbm, nodes_hbm, out, boundary, nodes, sems):
    copies = [pltpu.make_async_copy(boundary_hbm, boundary, sems.at[0]), pltpu.make_async_copy(nodes_hbm, nodes, sems.at[1])]
    for copy in copies:
        copy.start()
    for copy in copies:
        copy.wait()
    hot = ones_where(iota((nodes.shape[0], boundary.shape[1]), 0) == boundary[...])
    out[...] = dot_t(hot, nodes[...]).astype(BF)


def before_body(sender, receiver, nodes, w_in, edges, ready, out, table_r, table_s):
    n, f = nodes.shape

    @pl.when(pl.program_id(0) == 0)
    def _():
        table_s[...] = dot(nodes[...], w_in[0:f, :]).astype(BF)
        table_r[...] = dot(nodes[...], w_in[f : 2 * f, :]).astype(BF)

    total = dot(edges[...], w_in[2 * f : 3 * f, :])
    total += dot(rows_hot(sender[0], n), table_s[...])
    total += dot(rows_hot(receiver[0], n), table_r[...])
    out[...] = total


def grid_before_body(receiver, nodes, w_in, edges, ready, *refs):
    m = AHEAD_MESH
    ahead, out, near, table_r, sems = refs[:m], refs[m], refs[m + 1 : 2 * m + 1], refs[-2], refs[-1]
    n, f = nodes.shape

    @pl.when(pl.program_id(0) == 0)
    def _():
        ahead_of(ahead, near, sems)
        table_r[...] = dot(nodes[...], w_in[f : 2 * f, :]).astype(BF)

    out[...] = dot(edges[...], w_in[2 * f : 3 * f, :]) + dot(rows_hot(receiver[0], n), table_r[...])

    @pl.when(pl.program_id(0) == pl.num_programs(0) - 1)
    def _():
        for copy in ahead_of(ahead, near, sems, False):
            copy.wait()


def pieces_of(chips, offered):
    pair = 2 * offered
    far = [(2, 0), (-2, 1)]
    for step in range(STEPS + 1):
        far += [(LEAD + step, 0), (SEED + step, 0), (step - SEED, 1)]
    far += [(-LEAD, 1)]
    for step in range(1, STEPS + 1):
        far += [(-LEAD - step, 1), (-SEED - step, 1), (SEED - step, 0)]
    table = {}
    for i, (offset, flip) in enumerate(far):
        table.setdefault(offset % chips, (i * pair, flip))
    return table


def relative(sender, n, pair, chips, z, c):
    far = sender - n
    region = far // pair
    sign = 2 * c - 1
    offset = (sign * (region // 2 - z) + 2 * chips) % chips
    half = jnp.where(region % 2 == c, 0, 1)
    return far >= 0, region, offset, half, far % pair


def is_near(offset, chips):
    return (offset <= 1) | (offset == chips - 1)


def main_body(chips, first, place, live, sender, sender_row, receiver_row, need, w_s, both, up, down, edges, before, bias, w_out,
              gain, ready, *refs):
    totals, table = refs[-2:]
    z, c = place[0], place[1]
    n, _ = totals.shape
    step = pl.program_id(0)
    rows = edges.shape[0]
    pair, regions = need.shape
    offered = both.shape[0] // 2

    @pl.when(step == 0)
    def _():
        totals[...] = refs[0][...] if first else jnp.zeros_like(totals)
        r = iota((6 * pair, regions), 0)
        near = r // (2 * pair)
        half = (r // pair) % 2
        moved = jnp.where(near == 2, -1, near)
        chip = (z + (2 * c - 1) * moved + chips) % chips
        region = 2 * chip + jnp.where(half == 1, 1 - c, c)
        wanted = lax.dot_general(ones_where(iota((6 * pair, regions), 1) == region), need[...].astype(F32).astype(BF),
                                 (((1,), (1,)), ((), ())), preferred_element_type=F32)
        lane = iota((6 * pair, pair), 1) == iota((6 * pair, pair), 0) % pair
        column = jnp.sum(jnp.where(lane, wanted, 0.0), axis=1, keepdims=True).astype(I32)
        chosen = []
        for j, (source, flip) in enumerate(((both, 0), (up, 0), (down, 1))):
            own_half = iota((2 * pair, 2 * offered), 0) // pair
            at = (1 - own_half if flip else own_half) * offered + column[j * 2 * pair : (j + 1) * 2 * pair, :]
            chosen.append(dot(ones_where(iota((2 * pair, 2 * offered), 1) == at), source[...]))
        table[...] = dot(jnp.concatenate(chosen, axis=0).astype(BF), w_s[...]).astype(BF)

    remote, _, offset, half, slot = relative(sender[0], n, pair, chips, z, c)
    near = jnp.where(offset == chips - 1, 2, offset)
    place_of = jnp.where(remote & is_near(offset, chips), near * 2 * pair + half * pair + slot, -1)
    pre = before[...] + dot(rows_hot(place_of, 6 * pair), table[...])
    update = finish(pre, bias[...], w_out[...], gain[...])
    message = (edges[...].astype(F32) + update).astype(BF)
    position = (first + step) * rows + iota((1, rows), 1)
    remote, _, offset, _, _ = relative(sender_row[0], n, pair, chips, z, c)
    later = remote & jnp.logical_not(is_near(offset, chips))
    target = jnp.where((position < live[0]) & jnp.logical_not(later), receiver_row[0], -1)
    totals[...] += dot(ones_where(iota((n, rows), 0) == target), message)


def ahead_of(sources, targets, sems, begin=True):
    copies = [pltpu.make_async_copy(a.at[pl.ds(0, b.shape[0]), :], b, sems.at[i]) for i, (a, b) in enumerate(zip(sources, targets))]
    for copy in copies if begin else ():
        copy.start()
    return copies


def gathered(at, sources, starts):
    out = None
    for source, start in zip(sources, starts):
        hot = ones_where(iota((at.shape[0], source.shape[0]), 1) + start == at)
        part = dot(hot, source[...])
        out = part if out is None else out + part
    return out


def compact_body(chips, offered, starts, place, live, sender, receiver, need, w_e, table_r, edges, *refs):
    k, m = len(starts), AHEAD_FAR
    sources, ahead = refs[:k], refs[k : k + m]
    outs, count, near = refs[k + m : k + m + 5], refs[k + m + 5], refs[k + m + 6 : k + 2 * m + 6]
    ahead_sems = refs[-1]
    pre, rows, source_rows, at_out, target_out = outs
    fetches = ahead_of(ahead, near, ahead_sems)
    z, c = place[0], place[1]
    groups = sender.shape[0]
    n, _ = table_r.shape
    pair, regions = need.shape
    where_at = pieces_of(chips, offered)
    send = sender[...]
    remote, _, offset, _, _ = relative(send, n, pair, chips, z, c)
    position = iota((groups, 128), 0) * 128 + iota((groups, 128), 1)
    late = remote & jnp.logical_not(is_near(offset, chips)) & (position < live[0])
    late_bits = ones_where(late)
    within = dot(late_bits, ones_where(iota((128, 128), 0) < iota((128, 128), 1)))
    above = jnp.sum(dot(ones_where(iota((groups, groups), 1) < iota((groups, groups), 0)), late_bits), axis=1, keepdims=True)
    rank = jnp.where(late, (within + above).astype(I32), -1)
    total = jnp.sum(jnp.where(late, 1, 0))
    blocks = (total + LATE - 1) // LATE
    count[0] = blocks

    def one(block, carry):
        base = pl.multiple_of(block * LATE, LATE)
        lines = pl.ds(base, LATE)
        hot, send_at, receive_at = [], jnp.zeros((LATE, 128), I32), jnp.zeros((LATE, 128), I32)
        for g in range(groups):
            match = iota((LATE, 128), 0) + base == rank[g : g + 1, :]
            hot.append(ones_where(match))
            send_at += jnp.where(match, send[g : g + 1, :] + 1, 0)
            receive_at += jnp.where(match, receiver[g : g + 1, :] + 1, 0)
        edge = dot(jnp.concatenate(hot, axis=1), edges[...]).astype(BF)
        from_ = jnp.sum(send_at, axis=1, keepdims=True) - 1
        to = jnp.sum(receive_at, axis=1, keepdims=True) - 1
        valid, region, offset, half, slot = relative(from_, n, pair, chips, z, c)
        wanted = lax.dot_general(ones_where(iota((LATE, regions), 1) == region), need[...].astype(F32).astype(BF),
                                 (((1,), (1,)), ((), ())), preferred_element_type=F32)
        chosen = jnp.sum(jnp.where(iota((LATE, pair), 1) == slot, wanted, 0.0), axis=1, keepdims=True).astype(I32)
        start, flip = jnp.zeros((LATE, 1), I32), jnp.zeros((LATE, 1), I32)
        for key, (row, turned) in where_at.items():
            start = jnp.where(offset == key, row, start)
            flip = jnp.where(offset == key, turned, flip)
        at = jnp.where(valid, start + jnp.where(flip == 1, 1 - half, half) * offered + chosen, -1)
        rows[lines, :] = edge
        pre[lines, :] = dot(edge, w_e[...]) + dot(ones_where(iota((LATE, n), 1) == to), table_r[...])
        source_rows[lines, :] = gathered(at, sources, starts).astype(BF)
        at_out[lines, :] = jnp.broadcast_to(at, (LATE, 128))
        target_out[lines, :] = jnp.broadcast_to(to, (LATE, 128))
        return carry

    lax.fori_loop(0, blocks, one, 0)
    for fetch in fetches:
        fetch.wait()


def node_part_body(nodes, w_in, grid_nodes, grid_w_in, ready, out, grid_out):
    out[...] = dot(nodes[...], w_in[...])
    grid_out[...] = dot(grid_nodes[...], grid_w_in[...])


def far_body(starts, count, nodes, node_part, boundary, totals, bias, gain, node_bias, node_gain, w_s, w_out, node_in, node_out, *refs):
    k, m = len(starts), AHEAD_GRID
    sources, (pre, rows, source_rows, at, target), ahead = refs[:k], refs[k : k + 5], refs[k + 5 : k + 5 + m]
    result, kept_result, published = refs[k + 5 + m : k + 8 + m]
    near, acc, ahead_sems = refs[k + 8 + m : k + 8 + 2 * m], refs[-2], refs[-1]
    n, f = nodes.shape
    fetches = ahead_of(ahead, near, ahead_sems)
    acc[...] = totals[...]

    def one(block, carry):
        lines = pl.ds(pl.multiple_of(block * LATE, LATE), LATE)
        source = (source_rows[lines, :].astype(F32) + gathered(at[lines, :][:, 0:1], sources, starts)).astype(BF)
        update = finish(pre[lines, :] + dot(source, w_s[...]), bias[...], w_out[...], gain[...])
        message = (rows[lines, :].astype(F32) + update).astype(BF)
        eye = iota((128, 128), 0) == iota((128, 128), 1)
        targets = target[lines, :] + 1
        to = [jnp.sum(jnp.where(eye, targets[i : i + 128, :], 0), axis=0, keepdims=True) for i in range(0, LATE, 128)]
        acc[...] += dot(ones_where(iota((n, LATE), 0) + 1 == jnp.concatenate(to, axis=1)), message)
        return carry

    lax.fori_loop(0, count[0], one, 0)
    pre_node = node_part[...] + dot(acc[...].astype(BF), node_in[f : 2 * f, :])
    update = finish(pre_node, node_bias[...], node_out[...], node_gain[...])
    value = (nodes[...].astype(F32) + update).astype(BF)
    result[...] = value
    kept_result[...] = value
    hot = ones_where(iota((n, boundary.shape[1]), 0) == boundary[...])
    published[...] = dot_t(hot, value).astype(BF)
    for copy in fetches:
        copy.wait()


def grid_local_body(sender, mesh_out, w_s, before, out, table):
    n = mesh_out.shape[0]

    @pl.when(pl.program_id(0) == 0)
    def _():
        table[...] = dot(mesh_out[...], w_s[...]).astype(BF)

    out[...] = before[...] + dot(rows_hot(sender[0], n), table[...])


def grid_body(mesh_count, pair, sender, receiver_row, wanted, a, b, c, d, w_s, nodes, node_part, edges, before, bias, w_out, gain,
              node_in, node_bias, node_out, node_gain, result, totals, table):
    n, f = nodes.shape
    step = pl.program_id(0)
    rows = edges.shape[0]

    @pl.when(step == 0)
    def _():
        pieces = []
        for j, block in enumerate((a, b, c, d)):
            hot = ones_where(iota((block.shape[0], pair), 0) == wanted[j : j + 1, :])
            pieces.append(dot_t(hot, block[...]))
        chosen = jnp.concatenate(pieces, axis=0).astype(BF)
        table[...] = dot(chosen, w_s[...]).astype(BF)

    pre = before[...] + dot(rows_hot(sender[0] - mesh_count, table.shape[0]), table[...])
    update = finish(pre, bias[...], w_out[...], gain[...])
    message = (edges[...].astype(F32) + update).astype(BF)
    part = dot(ones_where(iota((n, rows), 0) == receiver_row[0]), message)

    @pl.when(step == 0)
    def _():
        totals[...] = part

    @pl.when(step > 0)
    def _():
        totals[...] += part

    @pl.when(step == pl.num_programs(0) - 1)
    def _():
        summed = totals[...].astype(BF)
        pre = node_part[...] + dot(summed, node_in[f : 2 * f, :])
        update = finish(pre, node_bias[...], node_out[...], node_gain[...])
        result[...] = (nodes[...].astype(F32) + update).astype(BF)


def local(
    mesh_nodes,
    mesh_edges,
    grid_nodes,
    grid_edges,
    boundary,
    mesh_need,
    mesh_sender,
    mesh_receiver,
    mesh_live,
    grid_need,
    grid_sender,
    grid_receiver,
    process_edge_in,
    process_edge_bias,
    process_edge_out,
    process_edge_gain,
    process_node_in,
    process_node_bias,
    process_node_out,
    process_node_gain,
    decode_edge_in,
    decode_edge_bias,
    decode_edge_out,
    decode_edge_gain,
    decode_node_in,
    decode_node_bias,
    decode_node_out,
    decode_node_gain,
):
    chips = lax.axis_size("z")
    regions = 2 * chips
    place = jnp.stack([lax.axis_index("z"), lax.axis_index("core")]).astype(I32)
    n, f = mesh_nodes.shape
    edges = mesh_edges.shape[0]
    grid_n = grid_nodes.shape[0]
    grid_e = grid_edges.shape[0]
    offered = boundary.shape[1]
    pair = mesh_need.shape[2]
    smem = pl.BlockSpec(memory_space=pltpu.SMEM)
    row = lambda v: v.reshape(1, -1)
    mesh_steps = edges // BLOCK
    grid_steps = grid_e // GRID_BLOCK
    as_blocks = lambda v, b: v.reshape(-1, b // 128, 128)
    as_rows = lambda v, b: v.reshape(-1, 1, b)
    idx_spec = lambda b: pl.BlockSpec((1, b // 128, 128), lambda i: (i, 0, 0))
    row_spec = lambda b: pl.BlockSpec((1, 1, b), lambda i: (i, 0, 0))
    tile = lambda b: pl.BlockSpec((b, f), lambda i: (i, 0))
    full = lambda v: (v, whole(v.shape))
    held = lambda v: (v, whole(v.shape), True)

    def along(steps):
        pairs = []
        for z in range(chips):
            pairs.append((2 * z, 2 * ((z + steps) % chips)))
            pairs.append((2 * z + 1, 2 * ((z - steps) % chips) + 1))
        return pairs

    def shift(v, steps):
        return lax.ppermute(v, REGION, along(steps))

    def swap(v):
        return lax.ppermute(v, "core", [(0, 1), (1, 0)])

    hbm = pl.BlockSpec(memory_space=HBM)
    anywhere = pl.BlockSpec(memory_space=pl.ANY)
    need = jnp.transpose(mesh_need[0])
    send_rows = mesh_sender.reshape(-1, 128)
    receive_rows = mesh_receiver.reshape(-1, 128)

    (own,) = call(publish_body, (1,), [(boundary, hbm), (mesh_nodes, hbm)], [((offered, f), BF, whole((offered, f)))],
                  [pltpu.VMEM((1, offered), I32), pltpu.VMEM((n, f), BF), pltpu.SemaphoreType.DMA((2,))],
                  flops=2 * offered * n * f, nbytes=2 * n * f)
    both = jnp.concatenate([own, swap(own)], axis=0)
    lead = [both]
    lead.append(shift(both, 1))
    seed = shift(both, SEED)
    lead.append(shift(lead[1], 1))
    lead.append(shift(lead[2], 1))
    back = [None]
    for k in range(1, LEAD + 1):
        back.append(swap(lead[k]))
    seed_back = swap(seed)
    vmem = lambda v: ((f if v is decode_edge_in else v.shape[0], f), v.dtype, pl.BlockSpec(memory_space=VMEM), VMEM)
    mesh_needs = [process_edge_in, mesh_nodes, mesh_edges, process_edge_out]
    grid_before, w_in_near, nodes_near, edges_near, out_near = call(
        grid_before_body, (grid_steps,),
        [(as_rows(grid_receiver, GRID_BLOCK), row_spec(GRID_BLOCK)), full(grid_nodes), full(decode_edge_in),
         (grid_edges, tile(GRID_BLOCK)), (lead[1], anywhere)] + [(v, hbm) for v in mesh_needs],
        [((grid_e, f), F32, tile(GRID_BLOCK), HBM)] + [vmem(v) for v in mesh_needs],
        [pltpu.VMEM((grid_n, f), BF), pltpu.SemaphoreType.DMA((AHEAD_MESH,))],
        flops=2 * f * f * (grid_e * 2 + grid_n), nbytes=6 * grid_e * f,
    )
    before, table_r = call(
        before_body, (mesh_steps,),
        [(as_blocks(mesh_sender, BLOCK), idx_spec(BLOCK)), (as_blocks(mesh_receiver, BLOCK), idx_spec(BLOCK)), held(nodes_near),
         held(w_in_near), (edges_near, tile(BLOCK), True), (lead[2], anywhere)],
        [((edges, f), F32, tile(BLOCK), VMEM), ((n, f), BF, whole((n, f)), VMEM)],
        [pltpu.VMEM((n, f), BF)],
        flops=2 * f * f * (edges * 3 + 2 * n), nbytes=6 * edges * f,
    )
    halves = mesh_steps // 2
    ready = lead[3]
    current = jnp.concatenate([lead[3], seed, seed_back], axis=0)
    chain, turned = [current], []
    for _ in range(STEPS):
        chain.append(shift(chain[-1], 1))
        turned.append(swap(chain[-1]))
    for part in range(2):
        first = part * halves
        at = lambda spec_rows, rank: pl.BlockSpec((1,) + spec_rows, lambda i: (i + first,) + (0,) * rank)
        moved = pl.BlockSpec((BLOCK, f), lambda i: (i + first, 0))
        (totals,) = call(
            functools.partial(main_body, chips, first), (halves,),
            [(place, smem), (mesh_live, smem), (as_blocks(mesh_sender, BLOCK), at((BLOCK // 128, 128), 2)),
             (as_rows(mesh_sender, BLOCK), at((1, BLOCK), 2)), (as_rows(mesh_receiver, BLOCK), at((1, BLOCK), 2)), full(need),
             (w_in_near, whole((f, f)), True), held(lead[0]), held(lead[1]), held(back[1]), (edges_near, moved, True),
             (before, moved, True), full(row(process_edge_bias)), held(out_near), full(row(process_edge_gain)),
             (ready, anywhere)] + ([held(totals)] if part else []),
            [((n, f), F32, whole((n, f)), VMEM)],
            [pltpu.VMEM((6 * pair, f), BF)],
            flops=2 * f * f * halves * BLOCK * 2, nbytes=6 * halves * BLOCK * f,
        )
        ready = chain[1]
    far = [lead[2], back[2]] + chain + [back[3]] + turned
    starts, at_row = [], 0
    for v in far:
        starts.append(at_row)
        at_row += v.shape[0]
    last = [STEPS + 2, len(far) - 2, len(far) - 1]
    early = [i for i in range(len(far)) if i not in last]
    far_needs = [process_node_in, process_node_out]
    grid_needs = [grid_before, decode_edge_in, grid_nodes, grid_edges, decode_edge_out, decode_node_in, decode_node_out]
    on_chip = lambda dtype, width: ((edges, width), dtype, pl.BlockSpec(memory_space=VMEM), VMEM)
    mesh_part, grid_part = call(
        node_part_body, (1,),
        [held(nodes_near), (process_node_in, whole((f, f))), full(grid_nodes), (decode_node_in, whole((f, f))),
         (chain[2], anywhere)],
        [((n, f), F32, whole((n, f)), VMEM), ((grid_n, f), F32, whole((grid_n, f)), VMEM)],
        flops=2 * f * f * (n + grid_n), nbytes=4 * n * f,
    )
    *stored, count, node_in_near, node_out_near = call(
        functools.partial(compact_body, chips, offered, tuple(starts[i] for i in early)), (1,),
        [(place, smem), (mesh_live, smem), full(send_rows), full(receive_rows), full(need),
         (w_in_near, pl.BlockSpec((f, f), lambda i: (2, 0)), True), held(table_r), held(edges_near)]
        + [held(far[i]) for i in early] + [(v, hbm) for v in far_needs],
        [on_chip(F32, f), on_chip(BF, f), on_chip(BF, f), on_chip(I32, 128), on_chip(I32, 128), ((1,), I32, smem)]
        + [vmem(v) for v in far_needs],
        [pltpu.SemaphoreType.DMA((AHEAD_FAR,))],
        flops=2 * f * 128 * (edges + 4 * f), nbytes=2 * edges * f,
    )
    mesh_out, mesh_kept, published, grid_before, grid_head, nodes_g, edges_g, out_g, node_in_g, node_out_g = call(
        functools.partial(far_body, tuple(starts[i] for i in last)), (1,),
        [(count, smem), held(nodes_near), held(mesh_part), full(boundary), held(totals), full(row(process_edge_bias)),
         full(row(process_edge_gain)), full(row(process_node_bias)), full(row(process_node_gain)), (w_in_near, whole((f, f)), True),
         held(out_near), held(node_in_near), held(node_out_near)] + [held(far[i]) for i in last]
        + [(v, pl.BlockSpec(memory_space=VMEM), True) for v in stored] + [(v, hbm) for v in grid_needs],
        [((n, f), BF, whole((n, f))), ((n, f), BF, whole((n, f)), VMEM), ((offered, f), BF, whole((offered, f)), VMEM)]
        + [vmem(v) for v in grid_needs],
        [pltpu.VMEM((n, f), F32), pltpu.SemaphoreType.DMA((AHEAD_GRID,))],
        flops=2 * f * f * 4 * n, nbytes=8 * n * f,
    )
    pieces = []
    for offset in (-2, -1, 1, 2):
        pieces.append(lax.ppermute(published, REGION, [(s, (s - offset) % regions) for s in range(regions)]))
    (grid_local,) = call(
        grid_local_body, (1,),
        [(as_rows(grid_sender, grid_e), row_spec(grid_e)), held(mesh_kept), held(grid_head),
         (grid_before, tile(grid_e), True)],
        [((grid_e, f), F32, tile(grid_e), VMEM)],
        [pltpu.VMEM((n, f), BF)],
        flops=2 * f * f * (grid_e + n), nbytes=8 * grid_e * f,
    )
    (grid_out,) = call(
        functools.partial(grid_body, n, pair), (1,),
        [(as_rows(grid_sender, grid_e), row_spec(grid_e)), (as_rows(grid_receiver, grid_e), row_spec(grid_e)),
         full(grid_need[0]), held(pieces[0]), held(pieces[1]), held(pieces[2]), held(pieces[3]),
         held(grid_head), held(nodes_g), held(grid_part), (edges_g, tile(grid_e), True), (grid_local, tile(grid_e), True),
         full(row(decode_edge_bias)), held(out_g), full(row(decode_edge_gain)), held(node_in_g),
         full(row(decode_node_bias)), held(node_out_g), full(row(decode_node_gain))],
        [((grid_n, f), BF, whole((grid_n, f)))],
        [pltpu.VMEM((grid_n, f), F32), pltpu.VMEM((4 * pair, f), BF)],
        flops=2 * f * f * (grid_e * 2 + 3 * grid_n), nbytes=6 * grid_e * f,
    )
    return (mesh_out, grid_out)


def solution(mesh):
    cores = 2
    finer = Mesh(
        mesh.devices.reshape(mesh.shape["member"], mesh.shape["region"] // cores, cores), ("member", "z", "core")
    )
    in_specs = (
        P(MEMBER_REGION, None),
        P(REGION, None),
        P(MEMBER_REGION, None),
        P(REGION, None),
        P(REGION, None),
        P(REGION, None, None),
        P(REGION, None),
        P(REGION, None),
        P(REGION),
        P(REGION, None, None),
        P(REGION, None),
        P(REGION, None),
    ) + (P(),) * 16
    out_specs = (P(MEMBER_REGION, None), P(MEMBER_REGION, None))

    return jax.shard_map(local, mesh=finer, in_specs=in_specs, out_specs=out_specs, check_vma=False)
```
